256 devices in a mesh: seg: 4 (over z_hi), ch: 64 (over x, y, z_lo, core).
Axes of the slice: x: 4, y: 4, z: 8 (z_hi: 4, z_lo: 2; z = z_hi * 2 + z_lo), core: 2. Of those that a mesh axis runs over, the one named last changes fastest.
Arguments:
- gate_in: bfloat16 [1536, 16384], P('ch', 'seg'), may hold values from -6 to 6
- key_in: bfloat16 [1536, 16384], P('ch', 'seg'), may hold values from -6 to 6
- value_in: bfloat16 [1536, 16384], P('ch', 'seg'), may hold values from -6 to 6
- kernel: float32 [1536, 16384], P('ch'), may hold values from -0.046875 to 0.046875
- skip_gain: float32 [1536], P('ch'), may hold values from -1 to 1
- out_weight: bfloat16 [1536, 1536], P('ch'), may hold values from -0.15625 to 0.15625
Outputs:
- output: bfloat16 [16384, 1536], P(('seg', 'ch'))
The draws below stay inside these ranges and needn't reach their ends.
All inputs are finite; a program needn't handle non-finite values.
Results may differ from the reference program's by a relative error of at most 0.0095.
Values may be sent and summed in bfloat16 or wider, within the bound.
A program may use at most 64 MiB of HBM per device.

```python
import jax
import jax.numpy as jnp
from jax import lax

D = 1536
SEQ = 16384


def level_of(rng, extent, cuts, least, top_value):
    level = 1.0
    for axis_at, shards_of in cuts:
        heights = jax.random.uniform(jax.random.fold_in(jax.random.fold_in(rng, 6), axis_at), (shards_of,), jnp.float32, least / len(cuts), top_value / len(cuts))
        level = level * jnp.repeat(jnp.exp(heights), extent[axis_at] // shards_of).reshape((-1,) + (1,) * (len(extent) - 1 - axis_at))
    return level


def bell_draw(key, extent, deviation, bound, split=(), dtype=jnp.bfloat16):
    drawn = deviation * jax.random.normal(key, extent, jnp.float32)
    if split:
        drawn = drawn * level_of(key, extent, split, -0.22, 0.18)
    return jnp.clip(drawn, -bound, bound).astype(dtype)


def setup_inputs(seed: int = 0) -> dict:
    key_list = jax.random.split(jax.random.key(seed), 7)
    gate_in = bell_draw(key_list[0], (D, SEQ), 1.0, 6.0, ((0, 64), (1, 4)))
    key_in = bell_draw(key_list[1], (D, SEQ), 1.0, 6.0, ((0, 64), (1, 4)))
    value_in = bell_draw(key_list[2], (D, SEQ), 1.0, 6.0, ((0, 64), (1, 4)))
    kernel = bell_draw(key_list[3], (D, SEQ), SEQ ** -0.5, 0.046875, ((0, 64),), jnp.float32)
    skip_gain = jnp.clip(jax.random.uniform(key_list[4], (D,), jnp.float32, -1.0, 1.0) * level_of(key_list[4], (D,), ((0, 64),), -0.4, 0.0), -1.0, 1.0)
    out_weight = bell_draw(key_list[5], (D, D), D ** -0.5, 0.15625, ((0, 64),))
    return dict(gate_in=gate_in, key_in=key_in, value_in=value_in, kernel=kernel, skip_gain=skip_gain, out_weight=out_weight)


def reference(gate_in, key_in, value_in, kernel, skip_gain, out_weight):
    mixed_in = key_in.astype(jnp.float32) * value_in.astype(jnp.float32)
    length = mixed_in.shape[1]
    product = jnp.fft.rfft(mixed_in, n=2 * length, axis=1) * jnp.fft.rfft(kernel, n=2 * length, axis=1)
    convolved = jnp.fft.irfft(product, n=2 * length, axis=1)[:, :length]
    gated = (gate_in.astype(jnp.float32) * (convolved + skip_gain[:, None] * mixed_in)).astype(jnp.bfloat16)
    result = lax.dot_general(gated, out_weight, (((0,), (0,)), ((), ())), preferred_element_type=jnp.float32)
    return result.astype(jnp.bfloat16)
```

```python
import math

import jax
import jax.numpy as jnp
import numpy as np
from jax import lax
from jax.experimental import pallas as pl
from jax.experimental.pallas import tpu as pltpu
from jax.sharding import PartitionSpec as P

MESH = pl.DeviceIdType.MESH
f32, bf16 = jnp.float32, jnp.bfloat16

SEGS = 4
NX, NY, NZ, CORES = 4, 4, 2, 2
CHIPS = NX * NY * NZ
L = 128
D = 1536
HERE = 24
OWN = HERE // SEGS
LOCAL = 4096
T = SEGS * LOCAL
TILES = LOCAL // L
PITCH = TILES + 8
KPITCH = T // L + 8
WIN = 16
CHUNKS = 4
COLS = D // CHUNKS
HALF = D // 2
PAIRS = OWN // 2
FAR_FIRST = (2, 1, 3)


def halves(table):
    high = table.astype(jnp.bfloat16)
    low = (table - high.astype(np.float32)).astype(jnp.bfloat16)
    return high, low


def tables():
    i = np.arange(L)
    outer = np.exp(-2j * np.pi * np.outer(i + 0.25, i) / L)
    twist = np.exp(-2j * np.pi * np.outer(i + 0.25, i) / T)
    inner = np.exp(-2j * np.pi * np.outer(i, i) / L)
    a2 = np.concatenate([outer.real, outer.imag], 0).astype(np.float32)
    d2 = np.block([[inner.real, inner.imag], [-inner.imag, inner.real]]).astype(np.float32)
    di = np.block([[inner.real, -inner.imag], [inner.imag, inner.real]]).astype(np.float32)
    a_high, a_low = halves(a2)
    d_high, d_low = halves(d2)
    back = (a2.T / T).astype(jnp.bfloat16)
    wide = np.concatenate([d_high, d_low, di.astype(jnp.bfloat16), back], 0)
    narrow = np.concatenate([a_high, a_low], 0)
    twiddle = np.concatenate([twist.real, twist.imag], 0).astype(np.float32)
    return wide, narrow, twiddle


def dot(a, b):
    return jnp.dot(a, b, preferred_element_type=f32)


def split(x):
    high = x.astype(bf16)
    return high, (x - high.astype(f32)).astype(bf16)


def kernel(
    gate_h, key_h, value_h, filt_h, skip_h, weight_h, wide_h, narrow_h, twiddle_h,
    out_ref,
    gate_v, key_v, value_v, filt_v, wide, narrow, twiddle,
    skip_s, strip, mixed_b, x_in, filt_x, spectrum, conv_out, conv_in, skip_v,
    outgoing, gathered, w_all, partial, partner,
    load_sem, x_send, x_recv, b_send, b_recv, w1_send, w1_recv,
    w2_send, w2_recv, w3_send, w3_recv, w4_send, w4_recv, w5_send, w5_recv,
    g_send, g_recv, p_send, p_recv,
):
    seg = lax.axis_index("seg")
    ch = lax.axis_index("ch")
    core = lax.rem(ch, CORES)
    chip = lax.div(ch, CORES)
    cx, cy, cz = lax.div(chip, NY * NZ), lax.rem(lax.div(chip, NZ), NY), lax.rem(chip, NZ)

    def at_seg(step):
        return lax.rem(seg + step, SEGS)

    def at_chip(other):
        return (seg, other * CORES + core)

    barrier = pltpu.get_barrier_semaphore()
    for step in range(1, SEGS):
        pl.semaphore_signal(barrier, inc=1, device_id=(at_seg(step), ch), device_id_type=MESH)
    other_core = (seg, chip * CORES + 1 - core)
    beside = chip + 1 - 2 * cz
    across = (lax.rem(seg + SEGS - 1 + 2 * cz, SEGS), beside * CORES + core)
    for device in (other_core, across):
        pl.semaphore_signal(barrier, inc=1, device_id=device, device_id_type=MESH)

    def greet(step, carry):
        pl.semaphore_signal(
            barrier, inc=1, device_id=at_chip(lax.rem(chip + step, CHIPS)), device_id_type=MESH
        )
        return carry

    lax.fori_loop(1, CHIPS, greet, 0)

    window = pl.multiple_of(lax.div(seg, 2) * 8, 8)
    loads = [
        pltpu.make_async_copy(src, dst, load_sem.at[n])
        for n, (src, dst) in enumerate(
            (
                (key_h, key_v),
                (value_h, value_v),
                (weight_h, w_all.at[0, 0, 0]),
                (filt_h.at[pl.ds(window, WIN), :], filt_v),
                (narrow_h, narrow),
                (twiddle_h, twiddle),
                (wide_h, wide),
                (gate_h, gate_v),
                (skip_h, skip_s),
            )
        )
    ]
    for load in loads:
        load.start()

    def rcopy(src, dst, send, recv, device):
        return pltpu.make_async_remote_copy(
            src_ref=src, dst_ref=dst, send_sem=send, recv_sem=recv, device_id=device, device_id_type=MESH
        )

    loads[0].wait()
    loads[1].wait()

    def mix(j, carry):
        cols = pl.ds(pl.multiple_of(j * L, L), L)
        product = key_v[:, cols].astype(f32) * value_v[:, cols].astype(f32)
        strip[pl.ds(j, HERE, stride=PITCH), :] = product
        return carry

    lax.fori_loop(0, TILES, mix, 0, unroll=4)
    for c in range(HERE):
        mixed_b[c] = strip[c * PITCH : c * PITCH + TILES, :].astype(bf16)

    pl.semaphore_wait(barrier, SEGS - 1 + 2 + CHIPS - 1)

    seg_rows = pl.ds(pl.multiple_of(seg * TILES, TILES), TILES)

    def x_copy(p, step):
        return rcopy(
            mixed_b.at[pl.ds(at_seg(step) * OWN + 2 * p, 2)],
            x_in.at[pl.ds(2 * p, 2), seg_rows, :],
            x_send.at[3 * p + step - 1],
            x_recv.at[3 * p + step - 1],
            (at_seg(step), ch),
        )

    left, right = pl.ds(0, HALF), pl.ds(HALF, HALF)
    z_copies = [
        rcopy(w_all.at[0, 0, 0, :, cols], w_all.at[1, 0, 0, :, cols], w1_send.at[n], w1_recv.at[n], device)
        for n, (cols, device) in enumerate(((left, at_chip(beside)), (right, across)))
    ]

    def x_peer(step):
        return at_chip((lax.rem(cx + step, NX) * NY + cy) * NZ + cz)

    def y_peer(step):
        return at_chip((cx * NY + lax.rem(cy + step, NY)) * NZ + cz)

    def first_copies(z, send, recv):
        own = w_all.at[z, 0, 0]
        return [
            rcopy(own, w_all.at[z, 0, NX - step], send.at[step - 1], recv.at[step - 1], x_peer(step))
            for step in range(1, NX)
        ] + [
            rcopy(own, w_all.at[z, NY - step, 0], send.at[step + 2], recv.at[step + 2], y_peer(step))
            for step in range(1, NY)
        ]

    def second_copies(z, send, recv):
        along_x, along_y = w_all.at[z, 0, 1:, :, left], w_all.at[z, 1:, 0, :, right]
        return [
            rcopy(along_x, w_all.at[z, NY - step, 1:, :, left], send.at[step - 1], recv.at[step - 1], y_peer(step))
            for step in range(1, NY)
        ] + [
            rcopy(along_y, w_all.at[z, 1:, NX - step, :, right], send.at[step + 2], recv.at[step + 2], x_peer(step))
            for step in range(1, NX)
        ]

    loads[2].wait()
    w_a = first_copies(0, w2_send, w2_recv)
    for p in range(PAIRS):
        for step in FAR_FIRST:
            x_copy(p, step).start()
        if p == 0:
            for copy in z_copies + w_a:
                copy.start()
    x_in[:, seg_rows, :] = mixed_b[pl.ds(seg * OWN, OWN)]

    loads[3].wait()
    for n in (4, 5, 6):
        loads[n].wait()

    def turn(j, carry):
        filt_x[pl.ds(j, WIN, stride=KPITCH), :] = filt_v[:, pl.ds(pl.multiple_of(j * L, L), L)]
        return carry

    lax.fori_loop(0, T // L, turn, 0, unroll=4)

    first = seg * OWN - window
    b_re, b_im = twiddle.at[:L, :], twiddle.at[L:, :]

    def spread(u, n):
        u_re, u_im = u[:L, n * L : (n + 1) * L], u[L:, n * L : (n + 1) * L]
        re, im = b_re[...], b_im[...]
        return jnp.concatenate([u_re * re - u_im * im, u_re * im + u_im * re], axis=1)

    def filter_spectrum(p, carry):
        strips = [
            filt_x[pl.ds(pl.multiple_of((first + 2 * p + n) * KPITCH, 8), T // L), :] for n in range(2)
        ]
        high, low = split(jnp.concatenate(strips, axis=1))
        a_high = narrow[: 2 * L, :]
        u = dot(a_high, high) + dot(narrow[2 * L :, :], high) + dot(a_high, low)
        v_high, v_low = split(jnp.concatenate([spread(u, n) for n in range(2)], axis=0))
        d_high = wide[: 2 * L, :]
        spectrum[p] = dot(v_high, d_high) + dot(v_low, d_high) + dot(v_high, wide[2 * L : 4 * L, :])
        return carry

    lax.fori_loop(0, PAIRS, filter_spectrum, 0)

    for copy in z_copies:
        copy.wait_recv()
    w_c = first_copies(1, w4_send, w4_recv)
    for copy in w_c:
        copy.start()
    for copy in w_a:
        copy.wait_recv()
    w_b = second_copies(0, w3_send, w3_recv)
    for copy in w_b:
        copy.start()

    def b_copy(p, step):
        rows = pl.ds(pl.multiple_of(at_seg(step) * TILES, TILES), TILES)
        return rcopy(
            conv_out.at[pl.ds(2 * p, 2), rows, :],
            conv_in.at[pl.ds(seg * OWN + 2 * p, 2)],
            b_send.at[3 * p + step - 1],
            b_recv.at[3 * p + step - 1],
            (at_seg(step), ch),
        )

    def convolve(p):
        u = dot(narrow[: 2 * L, :], jnp.concatenate([x_in[2 * p], x_in[2 * p + 1]], axis=1))
        v = jnp.concatenate([spread(u, n) for n in range(2)], axis=0)
        x = dot(v.astype(bf16), wide[: 2 * L, :])
        h = spectrum[p]
        x_re, x_im, h_re, h_im = x[:, :L], x[:, L:], h[:, :L], h[:, L:]
        z = jnp.concatenate([x_re * h_re - x_im * h_im, x_re * h_im + x_im * h_re], axis=1)
        e = dot(z.astype(bf16), wide[4 * L : 6 * L, :])
        columns = []
        for n in range(2):
            e_re, e_im = e[n * L : (n + 1) * L, :L], e[n * L : (n + 1) * L, L:]
            re, im = b_re[...], b_im[...]
            columns.append(jnp.concatenate([e_re * re + e_im * im, e_im * re - e_re * im], axis=0))
        y = dot(wide[6 * L :, :], jnp.concatenate(columns, axis=1).astype(bf16)).astype(bf16)
        conv_out[2 * p] = y[:, :L]
        conv_out[2 * p + 1] = y[:, L:]

    for p in range(PAIRS):
        for step in range(1, SEGS):
            x_copy(p, step).wait_recv()
        convolve(p)
        for step in FAR_FIRST:
            b_copy(p, step).start()
    for copy in w_c:
        copy.wait_recv()
    w_d = second_copies(1, w5_send, w5_recv)
    for copy in w_d:
        copy.start()
    conv_in[pl.ds(seg * OWN, OWN)] = conv_out[:, seg_rows, :]

    loads[7].wait()
    loads[8].wait()
    for c in range(HERE):
        skip_v[c : c + 1, :] = jnp.full((1, L), skip_s[c], f32)

    for p in range(PAIRS):
        for step in range(1, SEGS):
            b_copy(p, step).wait_recv()
    for c in range(HERE):
        strip[c * PITCH : c * PITCH + TILES, :] = conv_in[c].astype(f32)

    def gate_tile(j):
        cols = pl.ds(pl.multiple_of(j * L, L), L)
        mixed = key_v[:, cols].astype(f32) * value_v[:, cols].astype(f32)
        conv = strip[pl.ds(j, HERE, stride=PITCH), :]
        return (gate_v[:, cols].astype(f32) * (conv + skip_v[...] * mixed)).astype(bf16)

    gathered[:HERE, :] = gate_tile(chip)
    to_x = [lax.rem(cx + d, NX) * (NY * NZ) for d in range(NX)]
    to_y = [lax.rem(cy + d, NY) * NZ for d in range(NY)]
    to_z = [cz, 1 - cz]
    hops = sorted(
        ((dx, dy, dz) for dx in range(NX) for dy in range(NY) for dz in range(NZ) if dx or dy or dz),
        key=lambda d: -(min(d[0], NX - d[0]) + min(d[1], NY - d[1]) + d[2]),
    )
    sends = []
    for n, (dx, dy, dz) in enumerate(hops):
        target = to_x[dx] + to_y[dy] + to_z[dz]
        slot = (dz * NY + (NY - dy) % NY) * NX + (NX - dx) % NX
        outgoing[n] = gate_tile(target)
        sends.append(
            rcopy(
                outgoing.at[n], gathered.at[slot * HERE : (slot + 1) * HERE, :], g_send, g_recv, at_chip(target)
            )
        )
        if n:
            sends[n - 1].start()
    sends[-1].start()

    def wait_bytes(ref, sem):
        pltpu.make_async_copy(ref, ref, sem).wait()

    for copy in w_b + w_d:
        copy.wait_recv()
    others = pl.ds(HERE, (CHIPS - 1) * HERE)
    wait_bytes(gathered.at[others, :], g_recv)

    def p_copy(n):
        cols = pl.ds(n * COLS, COLS)
        return rcopy(
            partial.at[1 - core, :, cols],
            partner.at[:, cols],
            p_send.at[n],
            p_recv.at[n],
            other_core,
        )

    rows_here = L // CORES
    for n in range(CHUNKS):
        cols = pl.ds(n * COLS, COLS)
        sums = lax.dot_general(
            gathered[...],
            w_all[:, :, :, :, cols].reshape(CHIPS * HERE, COLS),
            (((0,), (0,)), ((), ())),
            preferred_element_type=f32,
        )
        partial[0, :, cols] = sums[:rows_here]
        partial[1, :, cols] = sums[rows_here:]
        if n:
            p_copy(n - 1).start()
    p_copy(CHUNKS - 1).start()
    for n in range(CHUNKS):
        cols = pl.ds(n * COLS, COLS)
        p_copy(n).wait_recv()
        out_ref[:, cols] = (partial[core, :, cols] + partner[:, cols]).astype(bf16)

    for p in range(PAIRS):
        for step in range(1, SEGS):
            x_copy(p, step).wait_send()
            b_copy(p, step).wait_send()
    for copy in z_copies + w_a + w_b + w_c + w_d:
        copy.wait_send()
    wait_bytes(gathered.at[others, :], g_send)
    for n in range(CHUNKS):
        p_copy(n).wait_send()


def on_device(*args):
    anywhere = pl.BlockSpec(memory_space=pltpu.HBM)
    wide, narrow, twiddle = tables()
    dma = pltpu.SemaphoreType.DMA
    return pl.pallas_call(
        kernel,
        out_shape=pltpu.VMEM((L // CORES, D), bf16),
        in_specs=[anywhere] * 9,
        out_specs=pl.BlockSpec(memory_space=pltpu.VMEM),
        scratch_shapes=[
            pltpu.VMEM((HERE, LOCAL), bf16),
            pltpu.VMEM((HERE, LOCAL), bf16),
            pltpu.VMEM((HERE, LOCAL), bf16),
            pltpu.VMEM((WIN, T), f32),
            pltpu.VMEM(wide.shape, bf16),
            pltpu.VMEM(narrow.shape, bf16),
            pltpu.VMEM(twiddle.shape, f32),
            pltpu.SMEM((HERE,), f32),
            pltpu.VMEM((HERE * PITCH, L), f32),
            pltpu.VMEM((HERE, TILES, L), bf16),
            pltpu.VMEM((OWN, T // L, L), bf16),
            pltpu.VMEM((WIN * KPITCH, L), f32),
            pltpu.VMEM((PAIRS, 2 * L, 2 * L), f32),
            pltpu.VMEM((OWN, T // L, L), bf16),
            pltpu.VMEM((HERE, TILES, L), bf16),
            pltpu.VMEM((HERE, L), f32),
            pltpu.VMEM((CHIPS, HERE, L), bf16),
            pltpu.VMEM((CHIPS * HERE, L), bf16),
            pltpu.VMEM((NZ, NY, NX, HERE, D), bf16),
            pltpu.VMEM((CORES, L // CORES, D), f32),
            pltpu.VMEM((L // CORES, D), f32),
            dma((9,)), dma((9,)), dma((9,)), dma((9,)), dma((9,)), dma((2,)), dma((2,)),
            dma((6,)), dma((6,)), dma((6,)), dma((6,)), dma((6,)), dma((6,)), dma((6,)), dma((6,)),
            dma, dma, dma((CHUNKS,)), dma((CHUNKS,)),
        ],
        compiler_params=pltpu.CompilerParams(
            collective_id=0, has_side_effects=True, vmem_limit_bytes=60 * 1024 * 1024
        ),
        name="layer",
    )(*args, jnp.asarray(wide), jnp.asarray(narrow), jnp.asarray(twiddle))


def solution(mesh):
    return jax.shard_map(
        on_device,
        mesh=mesh,
        in_specs=(P("ch", "seg"), P("ch", "seg"), P("ch", "seg"), P("ch", None), P("ch"), P("ch", None)),
        out_specs=P(("seg", "ch"), None),
        check_vma=False,
    )
```

```python
import math

import jax
import jax.numpy as jnp
import numpy as np
from jax import lax
from jax.experimental import pallas as pl
from jax.experimental.pallas import tpu as pltpu
from jax.sharding import PartitionSpec as P

MESH = pl.DeviceIdType.MESH
f32, bf16 = jnp.float32, jnp.bfloat16

SEGS = 4
NX, NY, NZ, CORES = 4, 4, 2, 2
CHIPS = NX * NY * NZ
L = 128
D = 1536
HERE = 24
OWN = HERE // SEGS
LOCAL = 4096
T = SEGS * LOCAL
TILES = LOCAL // L
PITCH = TILES + 8
KPITCH = T // L + 8
WIN = 16
CHUNKS = 4
COLS = D // CHUNKS
HALF = D // 2
PAIRS = OWN // 2
FAR_FIRST = (2, 1, 3)
ALL, NEAR = (1, 2, 3), (1, 3)


def halves(table):
    high = table.astype(jnp.bfloat16)
    low = (table - high.astype(np.float32)).astype(jnp.bfloat16)
    return high, low


def tables():
    i = np.arange(L)
    outer = np.exp(-2j * np.pi * np.outer(i + 0.25, i) / L)
    twist = np.exp(-2j * np.pi * np.outer(i + 0.25, i) / T)
    inner = np.exp(-2j * np.pi * np.outer(i, i) / L)
    a2 = np.concatenate([outer.real, outer.imag], 0).astype(np.float32)
    d2 = np.block([[inner.real, inner.imag], [-inner.imag, inner.real]]).astype(np.float32)
    di = np.block([[inner.real, -inner.imag], [inner.imag, inner.real]]).astype(np.float32)
    a_high, a_low = halves(a2)
    d_high, d_low = halves(d2)
    back = (a2.T / T).astype(jnp.bfloat16)
    wide = np.concatenate([d_high, d_low, di.astype(jnp.bfloat16), back], 0)
    narrow = np.concatenate([a_high, a_low], 0)
    twiddle = np.concatenate([twist.real, twist.imag], 0).astype(np.float32)
    return wide, narrow, twiddle


def dot(a, b):
    return jnp.dot(a, b, preferred_element_type=f32)


def split(x):
    high = x.astype(bf16)
    return high, (x - high.astype(f32)).astype(bf16)


def kernel(
    gate_h, key_h, value_h, filt_h, skip_h, weight_h, wide_h, narrow_h, twiddle_h,
    out_ref,
    gate_v, key_v, value_v, filt_v, wide, narrow, twiddle,
    skip_s, strip, mixed_b, x_in, filt_x, spectrum, conv_out, conv_in, skip_v,
    outgoing, gathered, w_all, partial, partner,
    load_sem, x_send, x_recv, b_send, b_recv, w1_send, w1_recv,
    w2_send, w2_recv, w3_send, w3_recv, w4_send, w4_recv, w5_send, w5_recv,
    g_send, g_recv, p_send, p_recv,
):
    seg = lax.axis_index("seg")
    ch = lax.axis_index("ch")
    core = lax.rem(ch, CORES)
    chip = lax.div(ch, CORES)
    cx, cy, cz = lax.div(chip, NY * NZ), lax.rem(lax.div(chip, NZ), NY), lax.rem(chip, NZ)

    def at_seg(step):
        return lax.rem(seg + step, SEGS)

    def at_chip(other):
        return (seg, other * CORES + core)

    barrier = pltpu.get_barrier_semaphore()
    for step in range(1, SEGS):
        pl.semaphore_signal(barrier, inc=1, device_id=(at_seg(step), ch), device_id_type=MESH)
    other_core = (seg, chip * CORES + 1 - core)
    beside = chip + 1 - 2 * cz
    across = (lax.rem(seg + SEGS - 1 + 2 * cz, SEGS), beside * CORES + core)
    for device in (other_core, across):
        pl.semaphore_signal(barrier, inc=1, device_id=device, device_id_type=MESH)

    to_x = [lax.rem(cx + d, NX) * (NY * NZ) for d in range(NX)]
    to_y = [lax.rem(cy + d, NY) * NZ for d in range(NY)]
    to_z = [cz, 1 - cz]
    hops = sorted(
        ((dx, dy, dz) for dx in range(NX) for dy in range(NY) for dz in range(NZ) if dx or dy or dz),
        key=lambda d: -(min(d[0], NX - d[0]) + min(d[1], NY - d[1]) + d[2]),
    )
    targets = [to_x[dx] + to_y[dy] + to_z[dz] for dx, dy, dz in hops]
    for target in targets:
        pl.semaphore_signal(barrier, inc=1, device_id=at_chip(target), device_id_type=MESH)

    window = pl.multiple_of(lax.div(seg, 2) * 8, 8)
    loads = [
        pltpu.make_async_copy(src, dst, load_sem.at[n])
        for n, (src, dst) in enumerate(
            (
                (key_h, key_v),
                (value_h, value_v),
                (weight_h, w_all.at[0, 0, 0]),
                (filt_h.at[pl.ds(window, WIN), :], filt_v),
                (narrow_h, narrow),
                (twiddle_h, twiddle),
                (wide_h, wide),
                (gate_h, gate_v),
                (skip_h, skip_s),
            )
        )
    ]
    for load in loads:
        load.start()

    def rcopy(src, dst, send, recv, device):
        return pltpu.make_async_remote_copy(
            src_ref=src, dst_ref=dst, send_sem=send, recv_sem=recv, device_id=device, device_id_type=MESH
        )

    loads[0].wait()
    loads[1].wait()

    def mix(j, carry):
        cols = pl.ds(pl.multiple_of(j * L, L), L)
        product = key_v[:, cols].astype(f32) * value_v[:, cols].astype(f32)
        strip[pl.ds(j, HERE, stride=PITCH), :] = product
        return carry

    lax.fori_loop(0, TILES, mix, 0, unroll=4)
    for c in range(HERE):
        mixed_b[c] = strip[c * PITCH : c * PITCH + TILES, :].astype(bf16)

    pl.semaphore_wait(barrier, SEGS - 1 + 2 + CHIPS - 1)

    seg_rows = pl.ds(pl.multiple_of(seg * TILES, TILES), TILES)

    def x_copy(p, step):
        return rcopy(
            mixed_b.at[pl.ds(at_seg(step) * OWN + 2 * p, 2)],
            x_in.at[pl.ds(2 * p, 2), seg_rows, :],
            x_send.at[3 * p + step - 1],
            x_recv.at[3 * p + step - 1],
            (at_seg(step), ch),
        )

    left, right = pl.ds(0, HALF), pl.ds(HALF, HALF)
    sides = (at_chip(beside), across)

    def z_pair(there, here, n):
        return [
            rcopy(here[m], there[m], w1_send.at[2 * n + m], w1_recv.at[2 * n + m], sides[m]) for m in range(2)
        ]

    def z_stage(n, *slots):
        return z_pair([w_all.at[(1, *slot)] for slot in slots], [w_all.at[(0, *slot)] for slot in slots], n)

    every = slice(None)
    z_copies = z_stage(0, (0, 0, every, left), (0, 0, every, right))
    z_far = z_stage(1, (0, 2), (2, 0))
    z_rest = z_stage(2, (2, slice(1, NX), every, left), (slice(1, NY), 2, every, right))

    def x_peer(step):
        return at_chip((lax.rem(cx + step, NX) * NY + cy) * NZ + cz)

    def y_peer(step):
        return at_chip((cx * NY + lax.rem(cy + step, NY)) * NZ + cz)

    def first_copies(z, steps, send, recv):
        own = w_all.at[z, 0, 0]
        return [
            rcopy(own, w_all.at[z, 0, NX - step], send.at[step - 1], recv.at[step - 1], x_peer(step))
            for step in steps
        ] + [
            rcopy(own, w_all.at[z, NY - step, 0], send.at[step + 2], recv.at[step + 2], y_peer(step))
            for step in steps
        ]

    def second_copies(z, steps, send, recv):
        along_x, along_y = w_all.at[z, 0, 1:, :, left], w_all.at[z, 1:, 0, :, right]
        return [
            rcopy(along_x, w_all.at[z, NY - step, 1:, :, left], send.at[step - 1], recv.at[step - 1], y_peer(step))
            for step in steps
        ] + [
            rcopy(along_y, w_all.at[z, 1:, NX - step, :, right], send.at[step + 2], recv.at[step + 2], x_peer(step))
            for step in steps
        ]

    loads[2].wait()
    w_a = first_copies(0, ALL, w2_send, w2_recv)
    for copy in z_copies + w_a:
        copy.start()
    for p in range(PAIRS):
        for step in FAR_FIRST:
            x_copy(p, step).start()
    x_in[:, seg_rows, :] = mixed_b[pl.ds(seg * OWN, OWN)]

    loads[3].wait()
    for n in (4, 5, 6):
        loads[n].wait()

    def turn(j, carry):
        filt_x[pl.ds(j, WIN, stride=KPITCH), :] = filt_v[:, pl.ds(pl.multiple_of(j * L, L), L)]
        return carry

    lax.fori_loop(0, T // L, turn, 0, unroll=4)

    first = seg * OWN - window
    b_re, b_im = twiddle.at[:L, :], twiddle.at[L:, :]

    def spread(u, n):
        u_re, u_im = u[:L, n * L : (n + 1) * L], u[L:, n * L : (n + 1) * L]
        re, im = b_re[...], b_im[...]
        return jnp.concatenate([u_re * re - u_im * im, u_re * im + u_im * re], axis=1)

    def filter_spectrum(p, carry):
        strips = [
            filt_x[pl.ds(pl.multiple_of((first + 2 * p + n) * KPITCH, 8), T // L), :] for n in range(2)
        ]
        high, low = split(jnp.concatenate(strips, axis=1))
        a_high = narrow[: 2 * L, :]
        u = dot(a_high, high) + dot(narrow[2 * L :, :], high) + dot(a_high, low)
        v_high, v_low = split(jnp.concatenate([spread(u, n) for n in range(2)], axis=0))
        d_high = wide[: 2 * L, :]
        spectrum[p] = dot(v_high, d_high) + dot(v_low, d_high) + dot(v_high, wide[2 * L : 4 * L, :])
        return carry

    lax.fori_loop(0, PAIRS, filter_spectrum, 0)

    for copy in z_copies:
        copy.wait_recv()
    w_c = first_copies(1, NEAR, w4_send, w4_recv)
    for copy in w_c:
        copy.start()
    for copy in w_a:
        copy.wait_recv()
    w_b = second_copies(0, ALL, w3_send, w3_recv)
    for copy in w_b + z_far:
        copy.start()

    def b_copy(p, step):
        rows = pl.ds(pl.multiple_of(at_seg(step) * TILES, TILES), TILES)
        return rcopy(
            conv_out.at[pl.ds(2 * p, 2), rows, :],
            conv_in.at[pl.ds(seg * OWN + 2 * p, 2)],
            b_send.at[3 * p + step - 1],
            b_recv.at[3 * p + step - 1],
            (at_seg(step), ch),
        )

    def convolve(p):
        u = dot(narrow[: 2 * L, :], jnp.concatenate([x_in[2 * p], x_in[2 * p + 1]], axis=1))
        v = jnp.concatenate([spread(u, n) for n in range(2)], axis=0)
        x = dot(v.astype(bf16), wide[: 2 * L, :])
        h = spectrum[p]
        x_re, x_im, h_re, h_im = x[:, :L], x[:, L:], h[:, :L], h[:, L:]
        z = jnp.concatenate([x_re * h_re - x_im * h_im, x_re * h_im + x_im * h_re], axis=1)
        e = dot(z.astype(bf16), wide[4 * L : 6 * L, :])
        columns = []
        for n in range(2):
            e_re, e_im = e[n * L : (n + 1) * L, :L], e[n * L : (n + 1) * L, L:]
            re, im = b_re[...], b_im[...]
            columns.append(jnp.concatenate([e_re * re + e_im * im, e_im * re - e_re * im], axis=0))
        y = dot(wide[6 * L :, :], jnp.concatenate(columns, axis=1).astype(bf16)).astype(bf16)
        conv_out[2 * p] = y[:, :L]
        conv_out[2 * p + 1] = y[:, L:]

    for p in range(PAIRS):
        for step in range(1, SEGS):
            x_copy(p, step).wait_recv()
        convolve(p)
        for step in FAR_FIRST:
            b_copy(p, step).start()
    for copy in w_c + z_far:
        copy.wait_recv()
    w_d = second_copies(1, NEAR, w5_send, w5_recv)
    for copy in w_d:
        copy.start()
    for copy in w_b:
        copy.wait_recv()
    for copy in z_rest:
        copy.start()
    conv_in[pl.ds(seg * OWN, OWN)] = conv_out[:, seg_rows, :]

    loads[7].wait()
    loads[8].wait()
    for c in range(HERE):
        skip_v[c : c + 1, :] = jnp.full((1, L), skip_s[c], f32)

    for p in range(PAIRS):
        for step in range(1, SEGS):
            b_copy(p, step).wait_recv()
    for c in range(HERE):
        strip[c * PITCH : c * PITCH + TILES, :] = conv_in[c].astype(f32)

    def gate_tile(j):
        cols = pl.ds(pl.multiple_of(j * L, L), L)
        mixed = key_v[:, cols].astype(f32) * value_v[:, cols].astype(f32)
        conv = strip[pl.ds(j, HERE, stride=PITCH), :]
        return (gate_v[:, cols].astype(f32) * (conv + skip_v[...] * mixed)).astype(bf16)

    gathered[:HERE, :] = gate_tile(chip)
    sends = []
    for n, (dx, dy, dz) in enumerate(hops):
        target = targets[n]
        slot = (dz * NY + (NY - dy) % NY) * NX + (NX - dx) % NX
        outgoing[n] = gate_tile(target)
        sends.append(
            rcopy(
                outgoing.at[n], gathered.at[slot * HERE : (slot + 1) * HERE, :], g_send, g_recv, at_chip(target)
            )
        )
        if n:
            sends[n - 1].start()
    sends[-1].start()

    def wait_bytes(ref, sem):
        pltpu.make_async_copy(ref, ref, sem).wait()

    for copy in w_d + z_rest:
        copy.wait_recv()
    others = pl.ds(HERE, (CHIPS - 1) * HERE)
    wait_bytes(gathered.at[others, :], g_recv)

    def p_copy(n):
        cols = pl.ds(n * COLS, COLS)
        return rcopy(
            partial.at[1 - core, :, cols],
            partner.at[:, cols],
            p_send.at[n],
            p_recv.at[n],
            other_core,
        )

    rows_here = L // CORES
    for n in range(CHUNKS):
        cols = pl.ds(n * COLS, COLS)
        sums = lax.dot_general(
            gathered[...],
            w_all[:, :, :, :, cols].reshape(CHIPS * HERE, COLS),
            (((0,), (0,)), ((), ())),
            preferred_element_type=f32,
        )
        partial[0, :, cols] = sums[:rows_here]
        partial[1, :, cols] = sums[rows_here:]
        if n:
            p_copy(n - 1).start()
    p_copy(CHUNKS - 1).start()
    for n in range(CHUNKS):
        cols = pl.ds(n * COLS, COLS)
        p_copy(n).wait_recv()
        out_ref[:, cols] = (partial[core, :, cols] + partner[:, cols]).astype(bf16)

    for p in range(PAIRS):
        for step in range(1, SEGS):
            x_copy(p, step).wait_send()
            b_copy(p, step).wait_send()
    for copy in z_copies + z_far + z_rest + w_a + w_b + w_c + w_d:
        copy.wait_send()
    wait_bytes(gathered.at[others, :], g_send)
    for n in range(CHUNKS):
        p_copy(n).wait_send()


def on_device(*args):
    anywhere = pl.BlockSpec(memory_space=pltpu.HBM)
    wide, narrow, twiddle = tables()
    dma = pltpu.SemaphoreType.DMA
    return pl.pallas_call(
        kernel,
        out_shape=pltpu.VMEM((L // CORES, D), bf16),
        in_specs=[anywhere] * 9,
        out_specs=pl.BlockSpec(memory_space=pltpu.VMEM),
        scratch_shapes=[
            pltpu.VMEM((HERE, LOCAL), bf16),
            pltpu.VMEM((HERE, LOCAL), bf16),
            pltpu.VMEM((HERE, LOCAL), bf16),
            pltpu.VMEM((WIN, T), f32),
            pltpu.VMEM(wide.shape, bf16),
            pltpu.VMEM(narrow.shape, bf16),
            pltpu.VMEM(twiddle.shape, f32),
            pltpu.SMEM((HERE,), f32),
            pltpu.VMEM((HERE * PITCH, L), f32),
            pltpu.VMEM((HERE, TILES, L), bf16),
            pltpu.VMEM((OWN, T // L, L), bf16),
            pltpu.VMEM((WIN * KPITCH, L), f32),
            pltpu.VMEM((PAIRS, 2 * L, 2 * L), f32),
            pltpu.VMEM((OWN, T // L, L), bf16),
            pltpu.VMEM((HERE, TILES, L), bf16),
            pltpu.VMEM((HERE, L), f32),
            pltpu.VMEM((CHIPS, HERE, L), bf16),
            pltpu.VMEM((CHIPS * HERE, L), bf16),
            pltpu.VMEM((NZ, NY, NX, HERE, D), bf16),
            pltpu.VMEM((CORES, L // CORES, D), f32),
            pltpu.VMEM((L // CORES, D), f32),
            dma((9,)), dma((9,)), dma((9,)), dma((9,)), dma((9,)), dma((6,)), dma((6,)),
            dma((6,)), dma((6,)), dma((6,)), dma((6,)), dma((6,)), dma((6,)), dma((6,)), dma((6,)),
            dma, dma, dma((CHUNKS,)), dma((CHUNKS,)),
        ],
        compiler_params=pltpu.CompilerParams(
            collective_id=0, has_side_effects=True, vmem_limit_bytes=60 * 1024 * 1024
        ),
        name="layer",
    )(*args, jnp.asarray(wide), jnp.asarray(narrow), jnp.asarray(twiddle))


def solution(mesh):
    return jax.shard_map(
        on_device,
        mesh=mesh,
        in_specs=(P("ch", "seg"), P("ch", "seg"), P("ch", "seg"), P("ch", None), P("ch"), P("ch", None)),
        out_specs=P(("seg", "ch"), None),
        check_vma=False,
    )
```

```python
import math

import jax
import jax.numpy as jnp
import numpy as np
from jax import lax
from jax.experimental import pallas as pl
from jax.experimental.pallas import tpu as pltpu
from jax.sharding import PartitionSpec as P

MESH = pl.DeviceIdType.MESH
f32, bf16 = jnp.float32, jnp.bfloat16

SEGS = 4
NX, NY, NZ, CORES = 4, 4, 2, 2
CHIPS = NX * NY * NZ
L = 128
D = 1536
HERE = 24
OWN = HERE // SEGS
LOCAL = 4096
T = SEGS * LOCAL
TILES = LOCAL // L
PITCH = TILES + 8
KPITCH = T // L + 8
WIN = 16
CHUNKS = 2
COLS = D // CHUNKS
HALF = D // 2
PAIRS = OWN // 2
FAR_FIRST = (2, 1, 3)
ALL, NEAR = (1, 2, 3), (1, 3)


def halves(table):
    high = table.astype(jnp.bfloat16)
    low = (table - high.astype(np.float32)).astype(jnp.bfloat16)
    return high, low


def tables():
    i = np.arange(L)
    outer = np.exp(-2j * np.pi * np.outer(i + 0.25, i) / L)
    twist = np.exp(-2j * np.pi * np.outer(i + 0.25, i) / T)
    inner = np.exp(-2j * np.pi * np.outer(i, i) / L)
    a2 = np.concatenate([outer.real, outer.imag], 0).astype(np.float32)
    d2 = np.block([[inner.real, inner.imag], [-inner.imag, inner.real]]).astype(np.float32)
    di = np.block([[inner.real, -inner.imag], [inner.imag, inner.real]]).astype(np.float32)
    a_high, a_low = halves(a2)
    d_high, d_low = halves(d2)
    back = (a2.T / T).astype(jnp.bfloat16)
    wide = np.concatenate([d_high, d_low, di.astype(jnp.bfloat16), back], 0)
    narrow = np.concatenate([a_high, a_low], 0)
    twiddle = np.concatenate([twist.real, twist.imag], 0).astype(np.float32)
    return wide, narrow, twiddle


def dot(a, b):
    return jnp.dot(a, b, preferred_element_type=f32)


def split(x):
    high = x.astype(bf16)
    return high, (x - high.astype(f32)).astype(bf16)


def kernel(
    gate_h, key_h, value_h, filt_h, skip_h, weight_h, wide_h, narrow_h, twiddle_h,
    out_ref,
    gate_v, key_v, value_v, filt_v, wide, narrow, twiddle,
    skip_s, strip, mixed_b, x_in, filt_x, spectrum, conv_out, conv_in, skip_v,
    outgoing, gathered, w_all, partial, partner,
    load_sem, x_send, x_recv, b_send, b_recv, w1_send, w1_recv,
    w2_send, w2_recv, w3_send, w3_recv, w4_send, w4_recv, w5_send, w5_recv,
    g_send, g_recv, p_send, p_recv,
):
    seg = lax.axis_index("seg")
    ch = lax.axis_index("ch")
    core = lax.rem(ch, CORES)
    chip = lax.div(ch, CORES)
    cx, cy, cz = lax.div(chip, NY * NZ), lax.rem(lax.div(chip, NZ), NY), lax.rem(chip, NZ)

    def at_seg(step):
        return lax.rem(seg + step, SEGS)

    def at_chip(other):
        return (seg, other * CORES + core)

    barrier = pltpu.get_barrier_semaphore()
    for step in range(1, SEGS):
        pl.semaphore_signal(barrier, inc=1, device_id=(at_seg(step), ch), device_id_type=MESH)
    other_core = (seg, chip * CORES + 1 - core)
    beside = chip + 1 - 2 * cz
    across = (lax.rem(seg + SEGS - 1 + 2 * cz, SEGS), beside * CORES + core)
    for device in (other_core, across):
        pl.semaphore_signal(barrier, inc=1, device_id=device, device_id_type=MESH)

    to_x = [lax.rem(cx + d, NX) * (NY * NZ) for d in range(NX)]
    to_y = [lax.rem(cy + d, NY) * NZ for d in range(NY)]
    to_z = [cz, 1 - cz]
    hops = sorted(
        ((dx, dy, dz) for dx in range(NX) for dy in range(NY) for dz in range(NZ) if dx or dy or dz),
        key=lambda d: -(min(d[0], NX - d[0]) + min(d[1], NY - d[1]) + d[2]),
    )
    targets = [to_x[dx] + to_y[dy] + to_z[dz] for dx, dy, dz in hops]
    for (dx, dy, dz), target in zip(hops, targets):
        if (dx > 0) + (dy > 0) + (dz > 0) == 1:
            pl.semaphore_signal(barrier, inc=1, device_id=at_chip(target), device_id_type=MESH)

    window = pl.multiple_of(lax.div(seg, 2) * 8, 8)
    loads = [
        pltpu.make_async_copy(src, dst, load_sem.at[n])
        for n, (src, dst) in enumerate(
            (
                (key_h, key_v),
                (value_h, value_v),
                (weight_h, w_all.at[0, 0, 0]),
                (filt_h.at[pl.ds(window, WIN), :], filt_v),
                (narrow_h, narrow),
                (twiddle_h, twiddle),
                (wide_h, wide),
                (gate_h, gate_v),
                (skip_h, skip_s),
            )
        )
    ]
    for load in loads:
        load.start()

    def rcopy(src, dst, send, recv, device):
        return pltpu.make_async_remote_copy(
            src_ref=src, dst_ref=dst, send_sem=send, recv_sem=recv, device_id=device, device_id_type=MESH
        )

    loads[0].wait()
    loads[1].wait()

    def mix(j, carry):
        cols = pl.ds(pl.multiple_of(j * L, L), L)
        product = key_v[:, cols].astype(f32) * value_v[:, cols].astype(f32)
        strip[pl.ds(j, HERE, stride=PITCH), :] = product
        return carry

    lax.fori_loop(0, TILES, mix, 0, unroll=4)
    for c in range(HERE):
        mixed_b[c] = strip[c * PITCH : c * PITCH + TILES, :].astype(bf16)

    pl.semaphore_wait(barrier, SEGS - 1 + 2 + NX - 1 + NY - 1 + NZ - 1)

    seg_rows = pl.ds(pl.multiple_of(seg * TILES, TILES), TILES)

    def x_copy(p, step):
        return rcopy(
            mixed_b.at[pl.ds(at_seg(step) * OWN + 2 * p, 2)],
            x_in.at[pl.ds(2 * p, 2), seg_rows, :],
            x_send.at[3 * p + step - 1],
            x_recv.at[3 * p + step - 1],
            (at_seg(step), ch),
        )

    left, right = pl.ds(0, HALF), pl.ds(HALF, HALF)
    sides = (at_chip(beside), across)

    def z_pair(there, here, n):
        return [
            rcopy(here[m], there[m], w1_send.at[2 * n + m], w1_recv.at[2 * n + m], sides[m]) for m in range(2)
        ]

    def z_stage(n, *slots):
        return z_pair([w_all.at[(1, *slot)] for slot in slots], [w_all.at[(0, *slot)] for slot in slots], n)

    every = slice(None)
    z_copies = z_stage(0, (0, 0, every, left), (0, 0, every, right))
    z_far = z_stage(1, (0, 2), (2, 0))
    z_rest = z_stage(2, (2, slice(1, NX), every, left), (slice(1, NY), 2, every, right))

    def x_peer(step):
        return at_chip((lax.rem(cx + step, NX) * NY + cy) * NZ + cz)

    def y_peer(step):
        return at_chip((cx * NY + lax.rem(cy + step, NY)) * NZ + cz)

    def first_copies(z, steps, send, recv):
        own = w_all.at[z, 0, 0]
        return [
            rcopy(own, w_all.at[z, 0, NX - step], send.at[step - 1], recv.at[step - 1], x_peer(step))
            for step in steps
        ] + [
            rcopy(own, w_all.at[z, NY - step, 0], send.at[step + 2], recv.at[step + 2], y_peer(step))
            for step in steps
        ]

    def second_copies(z, steps, send, recv):
        along_x, along_y = w_all.at[z, 0, 1:, :, left], w_all.at[z, 1:, 0, :, right]
        return [
            rcopy(along_x, w_all.at[z, NY - step, 1:, :, left], send.at[step - 1], recv.at[step - 1], y_peer(step))
            for step in steps
        ] + [
            rcopy(along_y, w_all.at[z, 1:, NX - step, :, right], send.at[step + 2], recv.at[step + 2], x_peer(step))
            for step in steps
        ]

    loads[2].wait()
    w_a = first_copies(0, ALL, w2_send, w2_recv)
    for copy in z_copies + w_a:
        copy.start()
    for p in range(PAIRS):
        for step in FAR_FIRST:
            x_copy(p, step).start()
    x_in[:, seg_rows, :] = mixed_b[pl.ds(seg * OWN, OWN)]

    loads[3].wait()
    for n in (4, 5, 6):
        loads[n].wait()

    def turn(j, carry):
        filt_x[pl.ds(j, WIN, stride=KPITCH), :] = filt_v[:, pl.ds(pl.multiple_of(j * L, L), L)]
        return carry

    lax.fori_loop(0, T // L, turn, 0, unroll=4)

    first = seg * OWN - window
    b_re, b_im = twiddle.at[:L, :], twiddle.at[L:, :]

    def spread(u, n):
        u_re, u_im = u[:L, n * L : (n + 1) * L], u[L:, n * L : (n + 1) * L]
        re, im = b_re[...], b_im[...]
        return jnp.concatenate([u_re * re - u_im * im, u_re * im + u_im * re], axis=1)

    def filter_spectrum(p, carry):
        strips = [
            filt_x[pl.ds(pl.multiple_of((first + 2 * p + n) * KPITCH, 8), T // L), :] for n in range(2)
        ]
        high, low = split(jnp.concatenate(strips, axis=1))
        a_high = narrow[: 2 * L, :]
        u = dot(a_high, high) + dot(narrow[2 * L :, :], high) + dot(a_high, low)
        v_high, v_low = split(jnp.concatenate([spread(u, n) for n in range(2)], axis=0))
        d_high = wide[: 2 * L, :]
        spectrum[p] = dot(v_high, d_high) + dot(v_low, d_high) + dot(v_high, wide[2 * L : 4 * L, :])
        return carry

    lax.fori_loop(0, PAIRS, filter_spectrum, 0)

    for copy in z_copies:
        copy.wait_recv()
    w_c = first_copies(1, NEAR, w4_send, w4_recv)
    for copy in w_c:
        copy.start()
    for copy in w_a:
        copy.wait_recv()
    w_b = second_copies(0, ALL, w3_send, w3_recv)
    for copy in w_b + z_far:
        copy.start()

    def b_copy(p, step):
        rows = pl.ds(pl.multiple_of(at_seg(step) * TILES, TILES), TILES)
        return rcopy(
            conv_out.at[pl.ds(2 * p, 2), rows, :],
            conv_in.at[pl.ds(seg * OWN + 2 * p, 2)],
            b_send.at[3 * p + step - 1],
            b_recv.at[3 * p + step - 1],
            (at_seg(step), ch),
        )

    def convolve(p):
        u = dot(narrow[: 2 * L, :], jnp.concatenate([x_in[2 * p], x_in[2 * p + 1]], axis=1))
        v = jnp.concatenate([spread(u, n) for n in range(2)], axis=0)
        x = dot(v.astype(bf16), wide[: 2 * L, :])
        h = spectrum[p]
        x_re, x_im, h_re, h_im = x[:, :L], x[:, L:], h[:, :L], h[:, L:]
        z = jnp.concatenate([x_re * h_re - x_im * h_im, x_re * h_im + x_im * h_re], axis=1)
        e = dot(z.astype(bf16), wide[4 * L : 6 * L, :])
        columns = []
        for n in range(2):
            e_re, e_im = e[n * L : (n + 1) * L, :L], e[n * L : (n + 1) * L, L:]
            re, im = b_re[...], b_im[...]
            columns.append(jnp.concatenate([e_re * re + e_im * im, e_im * re - e_re * im], axis=0))
        y = dot(wide[6 * L :, :], jnp.concatenate(columns, axis=1).astype(bf16)).astype(bf16)
        conv_out[2 * p] = y[:, :L]
        conv_out[2 * p + 1] = y[:, L:]

    for p in range(PAIRS):
        for step in range(1, SEGS):
            x_copy(p, step).wait_recv()
        convolve(p)
        for step in FAR_FIRST:
            b_copy(p, step).start()
    for copy in w_c + z_far:
        copy.wait_recv()
    w_d = second_copies(1, NEAR, w5_send, w5_recv)
    for copy in w_d:
        copy.start()
    conv_in[pl.ds(seg * OWN, OWN)] = conv_out[:, seg_rows, :]

    loads[7].wait()
    loads[8].wait()
    for c in range(HERE):
        skip_v[c : c + 1, :] = jnp.full((1, L), skip_s[c], f32)

    for p in range(PAIRS):
        for step in range(1, SEGS):
            b_copy(p, step).wait_recv()
    for c in range(HERE):
        strip[c * PITCH : c * PITCH + TILES, :] = conv_in[c].astype(f32)

    def gate_tile(j):
        cols = pl.ds(pl.multiple_of(j * L, L), L)
        mixed = key_v[:, cols].astype(f32) * value_v[:, cols].astype(f32)
        conv = strip[pl.ds(j, HERE, stride=PITCH), :]
        return (gate_v[:, cols].astype(f32) * (conv + skip_v[...] * mixed)).astype(bf16)

    gathered[:HERE, :] = gate_tile(chip)
    sends = []
    for n, (dx, dy, dz) in enumerate(hops):
        target = targets[n]
        slot = (dz * NY + (NY - dy) % NY) * NX + (NX - dx) % NX
        outgoing[n] = gate_tile(target)
        sends.append(
            rcopy(
                outgoing.at[n], gathered.at[slot * HERE : (slot + 1) * HERE, :], g_send, g_recv, at_chip(target)
            )
        )
        if n:
            sends[n - 1].start()
    sends[-1].start()

    for copy in w_b:
        copy.wait_recv()
    for copy in z_rest:
        copy.start()

    def wait_bytes(ref, sem):
        pltpu.make_async_copy(ref, ref, sem).wait()

    for copy in w_d + z_rest:
        copy.wait_recv()
    others = pl.ds(HERE, (CHIPS - 1) * HERE)
    wait_bytes(gathered.at[others, :], g_recv)

    def p_copy(n):
        cols = pl.ds(n * COLS, COLS)
        return rcopy(
            partial.at[1 - core, :, cols],
            partner.at[:, cols],
            p_send.at[n],
            p_recv.at[n],
            other_core,
        )

    rows_here = L // CORES
    turned = gathered[...].T
    for n in range(CHUNKS):
        cols = pl.ds(n * COLS, COLS)
        sums = lax.dot_general(
            turned,
            w_all[:, :, :, :, cols].reshape(CHIPS * HERE, COLS),
            (((1,), (0,)), ((), ())),
            preferred_element_type=f32,
        )
        partial[0, :, cols] = sums[:rows_here]
        partial[1, :, cols] = sums[rows_here:]
        if n:
            p_copy(n - 1).start()
    p_copy(CHUNKS - 1).start()
    for n in range(CHUNKS):
        cols = pl.ds(n * COLS, COLS)
        p_copy(n).wait_recv()
        out_ref[:, cols] = (partial[core, :, cols] + partner[:, cols]).astype(bf16)

    for p in range(PAIRS):
        for step in range(1, SEGS):
            x_copy(p, step).wait_send()
            b_copy(p, step).wait_send()
    for copy in z_copies + z_far + z_rest + w_a + w_b + w_c + w_d:
        copy.wait_send()
    wait_bytes(gathered.at[others, :], g_send)
    for n in range(CHUNKS):
        p_copy(n).wait_send()


def on_device(*args):
    anywhere = pl.BlockSpec(memory_space=pltpu.HBM)
    wide, narrow, twiddle = tables()
    dma = pltpu.SemaphoreType.DMA
    return pl.pallas_call(
        kernel,
        out_shape=pltpu.VMEM((L // CORES, D), bf16),
        in_specs=[anywhere] * 9,
        out_specs=pl.BlockSpec(memory_space=pltpu.VMEM),
        scratch_shapes=[
            pltpu.VMEM((HERE, LOCAL), bf16),
            pltpu.VMEM((HERE, LOCAL), bf16),
            pltpu.VMEM((HERE, LOCAL), bf16),
            pltpu.VMEM((WIN, T), f32),
            pltpu.VMEM(wide.shape, bf16),
            pltpu.VMEM(narrow.shape, bf16),
            pltpu.VMEM(twiddle.shape, f32),
            pltpu.SMEM((HERE,), f32),
            pltpu.VMEM((HERE * PITCH, L), f32),
            pltpu.VMEM((HERE, TILES, L), bf16),
            pltpu.VMEM((OWN, T // L, L), bf16),
            pltpu.VMEM((WIN * KPITCH, L), f32),
            pltpu.VMEM((PAIRS, 2 * L, 2 * L), f32),
            pltpu.VMEM((OWN, T // L, L), bf16),
            pltpu.VMEM((HERE, TILES, L), bf16),
            pltpu.VMEM((HERE, L), f32),
            pltpu.VMEM((CHIPS, HERE, L), bf16),
            pltpu.VMEM((CHIPS * HERE, L), bf16),
            pltpu.VMEM((NZ, NY, NX, HERE, D), bf16),
            pltpu.VMEM((CORES, L // CORES, D), f32),
            pltpu.VMEM((L // CORES, D), f32),
            dma((9,)), dma((9,)), dma((9,)), dma((9,)), dma((9,)), dma((6,)), dma((6,)),
            dma((6,)), dma((6,)), dma((6,)), dma((6,)), dma((6,)), dma((6,)), dma((6,)), dma((6,)),
            dma, dma, dma((CHUNKS,)), dma((CHUNKS,)),
        ],
        compiler_params=pltpu.CompilerParams(
            collective_id=0, has_side_effects=True, vmem_limit_bytes=60 * 1024 * 1024
        ),
        name="layer",
    )(*args, jnp.asarray(wide), jnp.asarray(narrow), jnp.asarray(twiddle))


def solution(mesh):
    return jax.shard_map(
        on_device,
        mesh=mesh,
        in_specs=(P("ch", "seg"), P("ch", "seg"), P("ch", "seg"), P("ch", None), P("ch"), P("ch", None)),
        out_specs=P(("seg", "ch"), None),
        check_vma=False,
    )
```

```python
import math

import jax
import jax.numpy as jnp
import numpy as np
from jax import lax
from jax.experimental import pallas as pl
from jax.experimental.pallas import tpu as pltpu
from jax.sharding import PartitionSpec as P

MESH = pl.DeviceIdType.MESH
f32, bf16 = jnp.float32, jnp.bfloat16

SEGS = 4
NX, NY, NZ, CORES = 4, 4, 2, 2
CHIPS = NX * NY * NZ
L = 128
D = 1536
HERE = 24
OWN = HERE // SEGS
LOCAL = 4096
T = SEGS * LOCAL
TILES = LOCAL // L
PITCH = TILES + 8
KPITCH = T // L + 8
WIN = 16
CHUNKS = 2
COLS = D // CHUNKS
HALF = D // 2
PAIRS = OWN // 2
FAR_FIRST = (2, 1, 3)
ALL, NEAR = (1, 2, 3), (1, 3)


def halves(table):
    high = table.astype(jnp.bfloat16)
    low = (table - high.astype(np.float32)).astype(jnp.bfloat16)
    return high, low


def tables():
    i = np.arange(L)
    outer = np.exp(-2j * np.pi * np.outer(i + 0.25, i) / L)
    twist = np.exp(-2j * np.pi * np.outer(i + 0.25, i) / T)
    inner = np.exp(-2j * np.pi * np.outer(i, i) / L)
    a2 = np.concatenate([outer.real, outer.imag], 0).astype(np.float32)
    d2 = np.block([[inner.real, inner.imag], [-inner.imag, inner.real]]).astype(np.float32)
    di = np.block([[inner.real, -inner.imag], [inner.imag, inner.real]]).astype(np.float32)
    a_high, a_low = halves(a2)
    d_high, d_low = halves(d2)
    back = (a2.T / T).astype(jnp.bfloat16)
    wide = np.concatenate([d_high, d_low, di.astype(jnp.bfloat16), back], 0)
    narrow = np.concatenate([a_high, a_low], 0)
    twiddle = np.concatenate([twist.real, twist.imag], 0).astype(np.float32)
    return wide, narrow, twiddle


def dot(a, b):
    return jnp.dot(a, b, preferred_element_type=f32)


def split(x):
    high = x.astype(bf16)
    return high, (x - high.astype(f32)).astype(bf16)


def kernel(
    gate_h, key_h, value_h, filt_h, skip_h, weight_h, wide_h, narrow_h, twiddle_h,
    out_ref,
    gate_v, key_v, value_v, filt_v, wide, narrow, twiddle,
    skip_s, strip, mixed_b, x_in, filt_x, spectrum, conv_out, conv_in, skip_v,
    outgoing, gathered, w_all, partial, leaving, partner,
    load_sem, x_send, x_recv, b_send, b_recv, w1_send, w1_recv,
    w2_send, w2_recv, w3_send, w3_recv, w4_send, w4_recv, w5_send, w5_recv,
    g_send, g_recv, p_send, p_recv,
):
    seg = lax.axis_index("seg")
    ch = lax.axis_index("ch")
    core = lax.rem(ch, CORES)
    chip = lax.div(ch, CORES)
    cx, cy, cz = lax.div(chip, NY * NZ), lax.rem(lax.div(chip, NZ), NY), lax.rem(chip, NZ)

    def at_seg(step):
        return lax.rem(seg + step, SEGS)

    def at_chip(other):
        return (seg, other * CORES + core)

    barrier = pltpu.get_barrier_semaphore()
    for step in range(1, SEGS):
        pl.semaphore_signal(barrier, inc=1, device_id=(at_seg(step), ch), device_id_type=MESH)
    other_core = (seg, chip * CORES + 1 - core)
    beside = chip + 1 - 2 * cz
    across = (lax.rem(seg + SEGS - 1 + 2 * cz, SEGS), beside * CORES + core)
    for device in (other_core, across):
        pl.semaphore_signal(barrier, inc=1, device_id=device, device_id_type=MESH)

    to_x = [lax.rem(cx + d, NX) * (NY * NZ) for d in range(NX)]
    to_y = [lax.rem(cy + d, NY) * NZ for d in range(NY)]
    to_z = [cz, 1 - cz]
    hops = sorted(
        ((dx, dy, dz) for dx in range(NX) for dy in range(NY) for dz in range(NZ) if dx or dy or dz),
        key=lambda d: -(min(d[0], NX - d[0]) + min(d[1], NY - d[1]) + d[2]),
    )
    targets = [to_x[dx] + to_y[dy] + to_z[dz] for dx, dy, dz in hops]
    for (dx, dy, dz), target in zip(hops, targets):
        if (dx > 0) + (dy > 0) + (dz > 0) == 1:
            pl.semaphore_signal(barrier, inc=1, device_id=at_chip(target), device_id_type=MESH)

    window = pl.multiple_of(lax.div(seg, 2) * 8, 8)
    loads = [
        pltpu.make_async_copy(src, dst, load_sem.at[n])
        for n, (src, dst) in enumerate(
            (
                (key_h, key_v),
                (value_h, value_v),
                (weight_h, w_all.at[0, 0, 0]),
                (filt_h.at[pl.ds(window, WIN), :], filt_v),
                (narrow_h, narrow),
                (twiddle_h, twiddle),
                (wide_h, wide),
                (gate_h, gate_v),
                (skip_h, skip_s),
            )
        )
    ]
    for load in loads:
        load.start()

    def rcopy(src, dst, send, recv, device):
        return pltpu.make_async_remote_copy(
            src_ref=src, dst_ref=dst, send_sem=send, recv_sem=recv, device_id=device, device_id_type=MESH
        )

    loads[0].wait()
    loads[1].wait()

    def mix(j, carry):
        cols = pl.ds(pl.multiple_of(j * L, L), L)
        product = key_v[:, cols].astype(f32) * value_v[:, cols].astype(f32)
        strip[pl.ds(j, HERE, stride=PITCH), :] = product
        return carry

    lax.fori_loop(0, TILES, mix, 0, unroll=4)
    for c in range(HERE):
        mixed_b[c] = strip[c * PITCH : c * PITCH + TILES, :].astype(bf16)

    pl.semaphore_wait(barrier, SEGS - 1 + 2 + NX - 1 + NY - 1 + NZ - 1)

    seg_rows = pl.ds(pl.multiple_of(seg * TILES, TILES), TILES)

    def x_copy(p, step):
        return rcopy(
            mixed_b.at[pl.ds(at_seg(step) * OWN + 2 * p, 2)],
            x_in.at[pl.ds(2 * p, 2), seg_rows, :],
            x_send.at[3 * p + step - 1],
            x_recv.at[3 * p + step - 1],
            (at_seg(step), ch),
        )

    left, right = pl.ds(0, HALF), pl.ds(HALF, HALF)
    sides = (at_chip(beside), across)

    def z_pair(there, here, n):
        return [
            rcopy(here[m], there[m], w1_send.at[2 * n + m], w1_recv.at[2 * n + m], sides[m]) for m in range(2)
        ]

    def z_stage(n, *slots):
        return z_pair([w_all.at[(1, *slot)] for slot in slots], [w_all.at[(0, *slot)] for slot in slots], n)

    every = slice(None)
    z_copies = z_stage(0, (0, 0, every, left), (0, 0, every, right))
    z_far = z_stage(1, (0, 2), (2, 0))
    z_rest = z_stage(2, (2, slice(1, NX), every, left), (slice(1, NY), 2, every, right))

    def x_peer(step):
        return at_chip((lax.rem(cx + step, NX) * NY + cy) * NZ + cz)

    def y_peer(step):
        return at_chip((cx * NY + lax.rem(cy + step, NY)) * NZ + cz)

    def first_copies(z, steps, send, recv):
        own = w_all.at[z, 0, 0]
        return [
            rcopy(own, w_all.at[z, 0, NX - step], send.at[step - 1], recv.at[step - 1], x_peer(step))
            for step in steps
        ] + [
            rcopy(own, w_all.at[z, NY - step, 0], send.at[step + 2], recv.at[step + 2], y_peer(step))
            for step in steps
        ]

    def second_copies(z, steps, send, recv):
        along_x, along_y = w_all.at[z, 0, 1:, :, left], w_all.at[z, 1:, 0, :, right]
        return [
            rcopy(along_x, w_all.at[z, NY - step, 1:, :, left], send.at[step - 1], recv.at[step - 1], y_peer(step))
            for step in steps
        ] + [
            rcopy(along_y, w_all.at[z, 1:, NX - step, :, right], send.at[step + 2], recv.at[step + 2], x_peer(step))
            for step in steps
        ]

    loads[2].wait()
    w_a = first_copies(0, ALL, w2_send, w2_recv)
    for copy in z_copies + w_a:
        copy.start()
    def x_start(*pairs):
        for p in pairs:
            for step in FAR_FIRST:
                x_copy(p, step).start()

    x_start(0)

    @pl.when(core == 0)
    def _():
        x_start(1, 2)

    x_in[:, seg_rows, :] = mixed_b[pl.ds(seg * OWN, OWN)]

    loads[3].wait()
    for n in (4, 5, 6):
        loads[n].wait()

    def turn(j, carry):
        filt_x[pl.ds(j, WIN, stride=KPITCH), :] = filt_v[:, pl.ds(pl.multiple_of(j * L, L), L)]
        return carry

    lax.fori_loop(0, T // L, turn, 0, unroll=4)

    first = seg * OWN - window
    b_re, b_im = twiddle.at[:L, :], twiddle.at[L:, :]

    def spread(u, n):
        u_re, u_im = u[:L, n * L : (n + 1) * L], u[L:, n * L : (n + 1) * L]
        re, im = b_re[...], b_im[...]
        return jnp.concatenate([u_re * re - u_im * im, u_re * im + u_im * re], axis=1)

    def filter_spectrum(p, carry):
        strips = [
            filt_x[pl.ds(pl.multiple_of((first + 2 * p + n) * KPITCH, 8), T // L), :] for n in range(2)
        ]
        high, low = split(jnp.concatenate(strips, axis=1))
        a_high = narrow[: 2 * L, :]
        u = dot(a_high, high) + dot(narrow[2 * L :, :], high) + dot(a_high, low)
        v_high, v_low = split(jnp.concatenate([spread(u, n) for n in range(2)], axis=0))
        d_high = wide[: 2 * L, :]
        spectrum[p] = dot(v_high, d_high) + dot(v_low, d_high) + dot(v_high, wide[2 * L : 4 * L, :])
        return carry

    lax.fori_loop(0, PAIRS, filter_spectrum, 0)

    @pl.when(core == 1)
    def _():
        x_start(1, 2)

    for copy in z_copies:
        copy.wait_recv()
    w_c = first_copies(1, NEAR, w4_send, w4_recv)
    for copy in w_c:
        copy.start()
    for copy in w_a:
        copy.wait_recv()
    w_b = second_copies(0, ALL, w3_send, w3_recv)
    for copy in w_b + z_far:
        copy.start()

    def b_copy(p, step):
        rows = pl.ds(pl.multiple_of(at_seg(step) * TILES, TILES), TILES)
        return rcopy(
            conv_out.at[pl.ds(2 * p, 2), rows, :],
            conv_in.at[pl.ds(seg * OWN + 2 * p, 2)],
            b_send.at[3 * p + step - 1],
            b_recv.at[3 * p + step - 1],
            (at_seg(step), ch),
        )

    def convolve(p):
        u = dot(narrow[: 2 * L, :], jnp.concatenate([x_in[2 * p], x_in[2 * p + 1]], axis=1))
        v = jnp.concatenate([spread(u, n) for n in range(2)], axis=0)
        x = dot(v.astype(bf16), wide[: 2 * L, :])
        h = spectrum[p]
        x_re, x_im, h_re, h_im = x[:, :L], x[:, L:], h[:, :L], h[:, L:]
        z = jnp.concatenate([x_re * h_re - x_im * h_im, x_re * h_im + x_im * h_re], axis=1)
        e = dot(z.astype(bf16), wide[4 * L : 6 * L, :])
        columns = []
        for n in range(2):
            e_re, e_im = e[n * L : (n + 1) * L, :L], e[n * L : (n + 1) * L, L:]
            re, im = b_re[...], b_im[...]
            columns.append(jnp.concatenate([e_re * re + e_im * im, e_im * re - e_re * im], axis=0))
        y = dot(wide[6 * L :, :], jnp.concatenate(columns, axis=1).astype(bf16)).astype(bf16)
        conv_out[2 * p] = y[:, :L]
        conv_out[2 * p + 1] = y[:, L:]

    for p in range(PAIRS):
        for step in range(1, SEGS):
            x_copy(p, step).wait_recv()
        convolve(p)
        for step in FAR_FIRST:
            b_copy(p, step).start()
    for copy in w_c + z_far:
        copy.wait_recv()
    w_d = second_copies(1, NEAR, w5_send, w5_recv)
    for copy in w_d:
        copy.start()
    conv_in[pl.ds(seg * OWN, OWN)] = conv_out[:, seg_rows, :]

    loads[7].wait()
    loads[8].wait()
    for c in range(HERE):
        skip_v[c : c + 1, :] = jnp.full((1, L), skip_s[c], f32)

    for p in range(PAIRS):
        for step in range(1, SEGS):
            b_copy(p, step).wait_recv()
    for c in range(HERE):
        strip[c * PITCH : c * PITCH + TILES, :] = conv_in[c].astype(f32)

    def gate_tile(j):
        cols = pl.ds(pl.multiple_of(j * L, L), L)
        mixed = key_v[:, cols].astype(f32) * value_v[:, cols].astype(f32)
        conv = strip[pl.ds(j, HERE, stride=PITCH), :]
        return (gate_v[:, cols].astype(f32) * (conv + skip_v[...] * mixed)).astype(bf16)

    gathered[:HERE, :] = gate_tile(chip)
    sends = []
    for n, (dx, dy, dz) in enumerate(hops):
        target = targets[n]
        slot = (dz * NY + (NY - dy) % NY) * NX + (NX - dx) % NX
        outgoing[n] = gate_tile(target)
        sends.append(
            rcopy(
                outgoing.at[n], gathered.at[slot * HERE : (slot + 1) * HERE, :], g_send, g_recv, at_chip(target)
            )
        )
        if n:
            sends[n - 1].start()
    sends[-1].start()

    for copy in w_b:
        copy.wait_recv()
    for copy in z_rest:
        copy.start()

    def wait_bytes(ref, sem):
        pltpu.make_async_copy(ref, ref, sem).wait()

    for copy in w_d + z_rest:
        copy.wait_recv()
    others = pl.ds(HERE, (CHIPS - 1) * HERE)
    wait_bytes(gathered.at[others, :], g_recv)

    def p_copy(n):
        cols = pl.ds(n * COLS, COLS)
        return rcopy(
            leaving.at[1 - core, :, cols],
            partner.at[:, cols],
            p_send.at[n],
            p_recv.at[n],
            other_core,
        )

    rows_here = L // CORES
    turned = gathered[...].T
    for n in range(CHUNKS):
        cols = pl.ds(n * COLS, COLS)
        sums = lax.dot_general(
            turned,
            w_all[:, :, :, :, cols].reshape(CHIPS * HERE, COLS),
            (((1,), (0,)), ((), ())),
            preferred_element_type=f32,
        )
        partial[0, :, cols] = sums[:rows_here]
        partial[1, :, cols] = sums[rows_here:]
        leaving[0, :, cols] = sums[:rows_here].astype(bf16)
        leaving[1, :, cols] = sums[rows_here:].astype(bf16)
        if n:
            p_copy(n - 1).start()
    p_copy(CHUNKS - 1).start()
    for n in range(CHUNKS):
        cols = pl.ds(n * COLS, COLS)
        p_copy(n).wait_recv()
        out_ref[:, cols] = (partial[core, :, cols] + partner[:, cols].astype(f32)).astype(bf16)

    for p in range(PAIRS):
        for step in range(1, SEGS):
            x_copy(p, step).wait_send()
            b_copy(p, step).wait_send()
    for copy in z_copies + z_far + z_rest + w_a + w_b + w_c + w_d:
        copy.wait_send()
    wait_bytes(gathered.at[others, :], g_send)
    for n in range(CHUNKS):
        p_copy(n).wait_send()


def on_device(*args):
    anywhere = pl.BlockSpec(memory_space=pltpu.HBM)
    wide, narrow, twiddle = tables()
    dma = pltpu.SemaphoreType.DMA
    return pl.pallas_call(
        kernel,
        out_shape=pltpu.VMEM((L // CORES, D), bf16),
        in_specs=[anywhere] * 9,
        out_specs=pl.BlockSpec(memory_space=pltpu.VMEM),
        scratch_shapes=[
            pltpu.VMEM((HERE, LOCAL), bf16),
            pltpu.VMEM((HERE, LOCAL), bf16),
            pltpu.VMEM((HERE, LOCAL), bf16),
            pltpu.VMEM((WIN, T), f32),
            pltpu.VMEM(wide.shape, bf16),
            pltpu.VMEM(narrow.shape, bf16),
            pltpu.VMEM(twiddle.shape, f32),
            pltpu.SMEM((HERE,), f32),
            pltpu.VMEM((HERE * PITCH, L), f32),
            pltpu.VMEM((HERE, TILES, L), bf16),
            pltpu.VMEM((OWN, T // L, L), bf16),
            pltpu.VMEM((WIN * KPITCH, L), f32),
            pltpu.VMEM((PAIRS, 2 * L, 2 * L), f32),
            pltpu.VMEM((OWN, T // L, L), bf16),
            pltpu.VMEM((HERE, TILES, L), bf16),
            pltpu.VMEM((HERE, L), f32),
            pltpu.VMEM((CHIPS, HERE, L), bf16),
            pltpu.VMEM((CHIPS * HERE, L), bf16),
            pltpu.VMEM((NZ, NY, NX, HERE, D), bf16),
            pltpu.VMEM((CORES, L // CORES, D), f32),
            pltpu.VMEM((CORES, L // CORES, D), bf16),
            pltpu.VMEM((L // CORES, D), bf16),
            dma((9,)), dma((9,)), dma((9,)), dma((9,)), dma((9,)), dma((6,)), dma((6,)),
            dma((6,)), dma((6,)), dma((6,)), dma((6,)), dma((6,)), dma((6,)), dma((6,)), dma((6,)),
            dma, dma, dma((CHUNKS,)), dma((CHUNKS,)),
        ],
        compiler_params=pltpu.CompilerParams(
            collective_id=0, has_side_effects=True, vmem_limit_bytes=60 * 1024 * 1024
        ),
        name="layer",
    )(*args, jnp.asarray(wide), jnp.asarray(narrow), jnp.asarray(twiddle))


def solution(mesh):
    return jax.shard_map(
        on_device,
        mesh=mesh,
        in_specs=(P("ch", "seg"), P("ch", "seg"), P("ch", "seg"), P("ch", None), P("ch"), P("ch", None)),
        out_specs=P(("seg", "ch"), None),
        check_vma=False,
    )
```

```python
import math

import jax
import jax.numpy as jnp
import numpy as np
from jax import lax
from jax.experimental import pallas as pl
from jax.experimental.pallas import tpu as pltpu
from jax.sharding import PartitionSpec as P

MESH = pl.DeviceIdType.MESH
f32, bf16 = jnp.float32, jnp.bfloat16

SEGS = 4
NX, NY, NZ, CORES = 4, 4, 2, 2
CHIPS = NX * NY * NZ
L = 128
D = 1536
HERE = 24
OWN = HERE // SEGS
LOCAL = 4096
T = SEGS * LOCAL
TILES = LOCAL // L
PITCH = TILES + 8
KPITCH = T // L + 8
WIN = 16
CHUNKS = 2
COLS = D // CHUNKS
HALF = D // 2
PAIRS = OWN // 2
FAR_FIRST = (2, 1, 3)
ALL, NEAR = (1, 2, 3), (1, 3)


def halves(table):
    high = table.astype(jnp.bfloat16)
    low = (table - high.astype(np.float32)).astype(jnp.bfloat16)
    return high, low


def tables():
    i = np.arange(L)
    outer = np.exp(-2j * np.pi * np.outer(i + 0.25, i) / L)
    twist = np.exp(-2j * np.pi * np.outer(i + 0.25, i) / T)
    inner = np.exp(-2j * np.pi * np.outer(i, i) / L)
    a2 = np.concatenate([outer.real, outer.imag], 0).astype(np.float32)
    d2 = np.block([[inner.real, inner.imag], [-inner.imag, inner.real]]).astype(np.float32)
    di = np.block([[inner.real, -inner.imag], [inner.imag, inner.real]]).astype(np.float32)
    a_high, a_low = halves(a2)
    d_high, d_low = halves(d2)
    back = (a2.T / T).astype(jnp.bfloat16)
    wide = np.concatenate([d_high, d_low, di.astype(jnp.bfloat16), back], 0)
    narrow = np.concatenate([a_high, a_low], 0)
    twiddle = np.concatenate([twist.real, twist.imag], 0).astype(np.float32)
    return wide, narrow, twiddle


def dot(a, b):
    return jnp.dot(a, b, preferred_element_type=f32)


def split(x):
    high = x.astype(bf16)
    return high, (x - high.astype(f32)).astype(bf16)


def kernel(
    gate_h, key_h, value_h, filt_h, skip_h, weight_h, wide_h, narrow_h, twiddle_h,
    out_ref,
    gate_v, key_v, value_v, filt_v, wide, narrow, twiddle,
    skip_s, strip, mixed_b, x_in, filt_x, spectrum, conv_out, conv_in, skip_v,
    outgoing, gathered, w_all, partial, leaving, partner,
    load_sem, x_send, x_recv, b_send, b_recv, w1_send, w1_recv,
    w2_send, w2_recv, w3_send, w3_recv, w4_send, w4_recv, w5_send, w5_recv,
    g_send, g_recv, p_send, p_recv,
):
    seg = lax.axis_index("seg")
    ch = lax.axis_index("ch")
    core = lax.rem(ch, CORES)
    chip = lax.div(ch, CORES)
    cx, cy, cz = lax.div(chip, NY * NZ), lax.rem(lax.div(chip, NZ), NY), lax.rem(chip, NZ)

    def at_seg(step):
        return lax.rem(seg + step, SEGS)

    def at_chip(other):
        return (seg, other * CORES + core)

    barrier = pltpu.get_barrier_semaphore()
    for step in range(1, SEGS):
        pl.semaphore_signal(barrier, inc=1, device_id=(at_seg(step), ch), device_id_type=MESH)
    other_core = (seg, chip * CORES + 1 - core)
    beside = chip + 1 - 2 * cz
    across = (lax.rem(seg + SEGS - 1 + 2 * cz, SEGS), beside * CORES + core)
    for device in (other_core, across):
        pl.semaphore_signal(barrier, inc=1, device_id=device, device_id_type=MESH)

    to_x = [lax.rem(cx + d, NX) * (NY * NZ) for d in range(NX)]
    to_y = [lax.rem(cy + d, NY) * NZ for d in range(NY)]
    to_z = [cz, 1 - cz]
    hops = sorted(
        ((dx, dy, dz) for dx in range(NX) for dy in range(NY) for dz in range(NZ) if dx or dy or dz),
        key=lambda d: -(min(d[0], NX - d[0]) + min(d[1], NY - d[1]) + d[2]),
    )
    targets = [to_x[dx] + to_y[dy] + to_z[dz] for dx, dy, dz in hops]
    for (dx, dy, dz), target in zip(hops, targets):
        if (dx > 0) + (dy > 0) + (dz > 0) == 1:
            pl.semaphore_signal(barrier, inc=1, device_id=at_chip(target), device_id_type=MESH)

    window = pl.multiple_of(lax.div(seg, 2) * 8, 8)
    loads = [
        pltpu.make_async_copy(src, dst, load_sem.at[n])
        for n, (src, dst) in enumerate(
            (
                (key_h, key_v),
                (value_h, value_v),
                (weight_h, w_all.at[0, 0, 0]),
                (filt_h.at[pl.ds(window, WIN), :], filt_v),
                (narrow_h, narrow),
                (twiddle_h, twiddle),
                (wide_h, wide),
                (gate_h, gate_v),
                (skip_h, skip_s),
            )
        )
    ]
    for load in loads:
        load.start()

    def rcopy(src, dst, send, recv, device):
        return pltpu.make_async_remote_copy(
            src_ref=src, dst_ref=dst, send_sem=send, recv_sem=recv, device_id=device, device_id_type=MESH
        )

    loads[0].wait()
    loads[1].wait()

    def mix(j, carry):
        cols = pl.ds(pl.multiple_of(j * L, L), L)
        product = key_v[:, cols].astype(f32) * value_v[:, cols].astype(f32)
        strip[pl.ds(j, HERE, stride=PITCH), :] = product
        return carry

    lax.fori_loop(0, TILES, mix, 0, unroll=4)
    for c in range(HERE):
        mixed_b[c] = strip[c * PITCH : c * PITCH + TILES, :].astype(bf16)

    pl.semaphore_wait(barrier, SEGS - 1 + 2 + NX - 1 + NY - 1 + NZ - 1)

    seg_rows = pl.ds(pl.multiple_of(seg * TILES, TILES), TILES)

    def x_copy(p, step):
        return rcopy(
            mixed_b.at[pl.ds(at_seg(step) * OWN + 2 * p, 2)],
            x_in.at[pl.ds(2 * p, 2), seg_rows, :],
            x_send.at[3 * p + step - 1],
            x_recv.at[3 * p + step - 1],
            (at_seg(step), ch),
        )

    left, right = pl.ds(0, HALF), pl.ds(HALF, HALF)
    sides = (at_chip(beside), across)

    def z_pair(there, here, n):
        return [
            rcopy(here[m], there[m], w1_send.at[2 * n + m], w1_recv.at[2 * n + m], sides[m]) for m in range(2)
        ]

    def z_stage(n, *slots):
        return z_pair([w_all.at[(1, *slot)] for slot in slots], [w_all.at[(0, *slot)] for slot in slots], n)

    every = slice(None)
    z_copies = z_stage(0, (0, 0, every, left), (0, 0, every, right))
    z_far = z_stage(1, (0, 2), (2, 0))
    z_rest = z_stage(2, (2, slice(1, NX), every, left), (slice(1, NY), 2, every, right))

    def x_peer(step):
        return at_chip((lax.rem(cx + step, NX) * NY + cy) * NZ + cz)

    def y_peer(step):
        return at_chip((cx * NY + lax.rem(cy + step, NY)) * NZ + cz)

    def first_copies(z, steps, send, recv):
        own = w_all.at[z, 0, 0]
        return [
            rcopy(own, w_all.at[z, 0, NX - step], send.at[step - 1], recv.at[step - 1], x_peer(step))
            for step in steps
        ] + [
            rcopy(own, w_all.at[z, NY - step, 0], send.at[step + 2], recv.at[step + 2], y_peer(step))
            for step in steps
        ]

    def second_copies(z, steps, send, recv):
        along_x, along_y = w_all.at[z, 0, 1:, :, left], w_all.at[z, 1:, 0, :, right]
        return [
            rcopy(along_x, w_all.at[z, NY - step, 1:, :, left], send.at[step - 1], recv.at[step - 1], y_peer(step))
            for step in steps
        ] + [
            rcopy(along_y, w_all.at[z, 1:, NX - step, :, right], send.at[step + 2], recv.at[step + 2], x_peer(step))
            for step in steps
        ]

    loads[2].wait()
    w_a = first_copies(0, ALL, w2_send, w2_recv)
    for copy in z_copies + w_a:
        copy.start()
    def x_start(*pairs):
        for p in pairs:
            for step in FAR_FIRST:
                x_copy(p, step).start()

    @pl.when(core == 0)
    def _():
        x_start(0)
        x_start(1, 2)

    x_in[:, seg_rows, :] = mixed_b[pl.ds(seg * OWN, OWN)]

    loads[3].wait()
    for n in (4, 5, 6):
        loads[n].wait()

    def turn(j, carry):
        filt_x[pl.ds(j, WIN, stride=KPITCH), :] = filt_v[:, pl.ds(pl.multiple_of(j * L, L), L)]
        return carry

    lax.fori_loop(0, T // L, turn, 0, unroll=4)

    @pl.when(core == 1)
    def _():
        x_start(0)

    first = seg * OWN - window
    b_re, b_im = twiddle.at[:L, :], twiddle.at[L:, :]

    def spread(u, n):
        u_re, u_im = u[:L, n * L : (n + 1) * L], u[L:, n * L : (n + 1) * L]
        re, im = b_re[...], b_im[...]
        return jnp.concatenate([u_re * re - u_im * im, u_re * im + u_im * re], axis=1)

    def filter_spectrum(p, carry):
        strips = [
            filt_x[pl.ds(pl.multiple_of((first + 2 * p + n) * KPITCH, 8), T // L), :] for n in range(2)
        ]
        high, low = split(jnp.concatenate(strips, axis=1))
        a_high = narrow[: 2 * L, :]
        u = dot(a_high, high) + dot(narrow[2 * L :, :], high) + dot(a_high, low)
        v_high, v_low = split(jnp.concatenate([spread(u, n) for n in range(2)], axis=0))
        d_high = wide[: 2 * L, :]
        spectrum[p] = dot(v_high, d_high) + dot(v_low, d_high) + dot(v_high, wide[2 * L : 4 * L, :])
        return carry

    lax.fori_loop(0, PAIRS, filter_spectrum, 0)

    @pl.when(core == 1)
    def _():
        x_start(1, 2)

    for copy in z_copies:
        copy.wait_recv()
    w_c = first_copies(1, NEAR, w4_send, w4_recv)
    for copy in w_c:
        copy.start()
    for copy in w_a:
        copy.wait_recv()
    w_b = second_copies(0, ALL, w3_send, w3_recv)
    for copy in w_b + z_far:
        copy.start()

    def b_copy(p, step):
        rows = pl.ds(pl.multiple_of(at_seg(step) * TILES, TILES), TILES)
        return rcopy(
            conv_out.at[pl.ds(2 * p, 2), rows, :],
            conv_in.at[pl.ds(seg * OWN + 2 * p, 2)],
            b_send.at[3 * p + step - 1],
            b_recv.at[3 * p + step - 1],
            (at_seg(step), ch),
        )

    def convolve(p):
        pair = range(2)
        us = [dot(narrow[: 2 * L, :], x_in[2 * p + n]) for n in pair]
        xs = [dot(spread(u, 0).astype(bf16), wide[: 2 * L, :]) for u in us]
        zs = []
        for n in pair:
            h, x = spectrum[p, n * L : (n + 1) * L, :], xs[n]
            x_re, x_im, h_re, h_im = x[:, :L], x[:, L:], h[:, :L], h[:, L:]
            zs.append(jnp.concatenate([x_re * h_re - x_im * h_im, x_re * h_im + x_im * h_re], axis=1))
        es = [dot(z.astype(bf16), wide[4 * L : 6 * L, :]) for z in zs]
        fs = []
        for e in es:
            e_re, e_im, re, im = e[:, :L], e[:, L:], b_re[...], b_im[...]
            fs.append(jnp.concatenate([e_re * re + e_im * im, e_im * re - e_re * im], axis=0).astype(bf16))
        for n in pair:
            conv_out[2 * p + n] = dot(wide[6 * L :, :], fs[n]).astype(bf16)

    for p in range(PAIRS):
        for step in range(1, SEGS):
            x_copy(p, step).wait_recv()
        convolve(p)
        for step in FAR_FIRST:
            b_copy(p, step).start()
    for copy in w_c + z_far:
        copy.wait_recv()
    w_d = second_copies(1, NEAR, w5_send, w5_recv)
    for copy in w_d:
        copy.start()
    conv_in[pl.ds(seg * OWN, OWN)] = conv_out[:, seg_rows, :]

    loads[7].wait()
    loads[8].wait()
    for c in range(HERE):
        skip_v[c : c + 1, :] = jnp.full((1, L), skip_s[c], f32)

    for p in range(PAIRS):
        for step in range(1, SEGS):
            b_copy(p, step).wait_recv()
        for c in range(HERE):
            if c % OWN // 2 == p:
                strip[c * PITCH : c * PITCH + TILES, :] = conv_in[c].astype(f32)

    def gate_tile(j):
        cols = pl.ds(pl.multiple_of(j * L, L), L)
        mixed = key_v[:, cols].astype(f32) * value_v[:, cols].astype(f32)
        conv = strip[pl.ds(j, HERE, stride=PITCH), :]
        return (gate_v[:, cols].astype(f32) * (conv + skip_v[...] * mixed)).astype(bf16)

    gathered[:HERE, :] = gate_tile(chip)
    sends = []
    for n, (dx, dy, dz) in enumerate(hops):
        target = targets[n]
        slot = (dz * NY + (NY - dy) % NY) * NX + (NX - dx) % NX
        outgoing[n] = gate_tile(target)
        sends.append(
            rcopy(
                outgoing.at[n], gathered.at[slot * HERE : (slot + 1) * HERE, :], g_send, g_recv, at_chip(target)
            )
        )
        if n:
            sends[n - 1].start()
    sends[-1].start()

    for copy in w_b:
        copy.wait_recv()
    for copy in z_rest:
        copy.start()

    def wait_bytes(ref, sem):
        pltpu.make_async_copy(ref, ref, sem).wait()

    for copy in w_d + z_rest:
        copy.wait_recv()
    others = pl.ds(HERE, (CHIPS - 1) * HERE)
    wait_bytes(gathered.at[others, :], g_recv)

    def p_copy(n):
        cols = pl.ds(n * COLS, COLS)
        return rcopy(
            leaving.at[1 - core, :, cols],
            partner.at[:, cols],
            p_send.at[n],
            p_recv.at[n],
            other_core,
        )

    rows_here = L // CORES
    turned = gathered[...].T
    for n in range(CHUNKS):
        cols = pl.ds(n * COLS, COLS)
        sums = lax.dot_general(
            turned,
            w_all[:, :, :, :, cols].reshape(CHIPS * HERE, COLS),
            (((1,), (0,)), ((), ())),
            preferred_element_type=f32,
        )
        partial[0, :, cols] = sums[:rows_here]
        partial[1, :, cols] = sums[rows_here:]
        leaving[0, :, cols] = sums[:rows_here].astype(bf16)
        leaving[1, :, cols] = sums[rows_here:].astype(bf16)
        if n:
            p_copy(n - 1).start()
    p_copy(CHUNKS - 1).start()
    for n in range(CHUNKS):
        cols = pl.ds(n * COLS, COLS)
        p_copy(n).wait_recv()
        out_ref[:, cols] = (partial[core, :, cols] + partner[:, cols].astype(f32)).astype(bf16)

    for p in range(PAIRS):
        for step in range(1, SEGS):
            x_copy(p, step).wait_send()
            b_copy(p, step).wait_send()
    for copy in z_copies + z_far + z_rest + w_a + w_b + w_c + w_d:
        copy.wait_send()
    wait_bytes(gathered.at[others, :], g_send)
    for n in range(CHUNKS):
        p_copy(n).wait_send()


def on_device(*args):
    anywhere = pl.BlockSpec(memory_space=pltpu.HBM)
    wide, narrow, twiddle = tables()
    dma = pltpu.SemaphoreType.DMA
    return pl.pallas_call(
        kernel,
        out_shape=pltpu.VMEM((L // CORES, D), bf16),
        in_specs=[anywhere] * 9,
        out_specs=pl.BlockSpec(memory_space=pltpu.VMEM),
        scratch_shapes=[
            pltpu.VMEM((HERE, LOCAL), bf16),
            pltpu.VMEM((HERE, LOCAL), bf16),
            pltpu.VMEM((HERE, LOCAL), bf16),
            pltpu.VMEM((WIN, T), f32),
            pltpu.VMEM(wide.shape, bf16),
            pltpu.VMEM(narrow.shape, bf16),
            pltpu.VMEM(twiddle.shape, f32),
            pltpu.SMEM((HERE,), f32),
            pltpu.VMEM((HERE * PITCH, L), f32),
            pltpu.VMEM((HERE, TILES, L), bf16),
            pltpu.VMEM((OWN, T // L, L), bf16),
            pltpu.VMEM((WIN * KPITCH, L), f32),
            pltpu.VMEM((PAIRS, 2 * L, 2 * L), f32),
            pltpu.VMEM((OWN, T // L, L), bf16),
            pltpu.VMEM((HERE, TILES, L), bf16),
            pltpu.VMEM((HERE, L), f32),
            pltpu.VMEM((CHIPS, HERE, L), bf16),
            pltpu.VMEM((CHIPS * HERE, L), bf16),
            pltpu.VMEM((NZ, NY, NX, HERE, D), bf16),
            pltpu.VMEM((CORES, L // CORES, D), f32),
            pltpu.VMEM((CORES, L // CORES, D), bf16),
            pltpu.VMEM((L // CORES, D), bf16),
            dma((9,)), dma((9,)), dma((9,)), dma((9,)), dma((9,)), dma((6,)), dma((6,)),
            dma((6,)), dma((6,)), dma((6,)), dma((6,)), dma((6,)), dma((6,)), dma((6,)), dma((6,)),
            dma, dma, dma((CHUNKS,)), dma((CHUNKS,)),
        ],
        compiler_params=pltpu.CompilerParams(
            collective_id=0, has_side_effects=True, vmem_limit_bytes=60 * 1024 * 1024
        ),
        name="layer",
    )(*args, jnp.asarray(wide), jnp.asarray(narrow), jnp.asarray(twiddle))


def solution(mesh):
    return jax.shard_map(
        on_device,
        mesh=mesh,
        in_specs=(P("ch", "seg"), P("ch", "seg"), P("ch", "seg"), P("ch", None), P("ch"), P("ch", None)),
        out_specs=P(("seg", "ch"), None),
        check_vma=False,
    )
```

```python
import math

import jax
import jax.numpy as jnp
import numpy as np
from jax import lax
from jax.experimental import pallas as pl
from jax.experimental.pallas import tpu as pltpu
from jax.sharding import PartitionSpec as P

MESH = pl.DeviceIdType.MESH
f32, bf16 = jnp.float32, jnp.bfloat16

SEGS = 4
NX, NY, NZ, CORES = 4, 4, 2, 2
CHIPS = NX * NY * NZ
L = 128
D = 1536
HERE = 24
OWN = HERE // SEGS
LOCAL = 4096
T = SEGS * LOCAL
TILES = LOCAL // L
PITCH = TILES + 8
KPITCH = T // L + 8
WIN = 16
CHUNKS = 2
COLS = D // CHUNKS
HALF = D // 2
PAIRS = OWN // 2
FAR_FIRST = (2, 1, 3)
ALL, NEAR = (1, 2, 3), (1, 3)


def halves(table):
    high = table.astype(jnp.bfloat16)
    low = (table - high.astype(np.float32)).astype(jnp.bfloat16)
    return high, low


def tables():
    i = np.arange(L)
    outer = np.exp(-2j * np.pi * np.outer(i + 0.25, i) / L)
    twist = np.exp(-2j * np.pi * np.outer(i + 0.25, i) / T)
    inner = np.exp(-2j * np.pi * np.outer(i, i) / L)
    a2 = np.concatenate([outer.real, outer.imag], 0).astype(np.float32)
    d2 = np.block([[inner.real, inner.imag], [-inner.imag, inner.real]]).astype(np.float32)
    di = np.block([[inner.real, -inner.imag], [inner.imag, inner.real]]).astype(np.float32)
    a_high, a_low = halves(a2)
    d_high, d_low = halves(d2)
    back = (a2.T / T).astype(jnp.bfloat16)
    wide = np.concatenate([d_high, d_low, di.astype(jnp.bfloat16), back], 0)
    narrow = np.concatenate([a_high, a_low], 0)
    twiddle = np.concatenate([twist.real, twist.imag], 0).astype(np.float32)
    return wide, narrow, twiddle


def dot(a, b):
    return jnp.dot(a, b, preferred_element_type=f32)


def split(x):
    high = x.astype(bf16)
    return high, (x - high.astype(f32)).astype(bf16)


def kernel(
    gate_h, key_h, value_h, filt_h, skip_h, weight_h, wide_h, narrow_h, twiddle_h,
    out_ref,
    gate_v, key_v, value_v, filt_v, wide, narrow, twiddle,
    skip_s, strip, mixed_b, x_in, filt_x, spectrum, conv_out, conv_in, skip_v,
    outgoing, gathered, w_all, partial, leaving, partner,
    load_sem, x_send, x_recv, b_send, b_recv, w1_send, w1_recv,
    w2_send, w2_recv, w3_send, w3_recv, w4_send, w4_recv, w5_send, w5_recv,
    g_send, g_recv, p_send, p_recv,
):
    seg = lax.axis_index("seg")
    ch = lax.axis_index("ch")
    core = lax.rem(ch, CORES)
    chip = lax.div(ch, CORES)
    cx, cy, cz = lax.div(chip, NY * NZ), lax.rem(lax.div(chip, NZ), NY), lax.rem(chip, NZ)

    def at_seg(step):
        return lax.rem(seg + step, SEGS)

    def at_chip(other):
        return (seg, other * CORES + core)

    barrier = pltpu.get_barrier_semaphore()
    for step in range(1, SEGS):
        pl.semaphore_signal(barrier, inc=1, device_id=(at_seg(step), ch), device_id_type=MESH)
    other_core = (seg, chip * CORES + 1 - core)
    beside = chip + 1 - 2 * cz
    across = (lax.rem(seg + SEGS - 1 + 2 * cz, SEGS), beside * CORES + core)
    for device in (other_core, across):
        pl.semaphore_signal(barrier, inc=1, device_id=device, device_id_type=MESH)

    to_x = [lax.rem(cx + d, NX) * (NY * NZ) for d in range(NX)]
    to_y = [lax.rem(cy + d, NY) * NZ for d in range(NY)]
    to_z = [cz, 1 - cz]
    hops = sorted(
        ((dx, dy, dz) for dx in range(NX) for dy in range(NY) for dz in range(NZ) if dx or dy or dz),
        key=lambda d: -(min(d[0], NX - d[0]) + min(d[1], NY - d[1]) + d[2]),
    )
    targets = [to_x[dx] + to_y[dy] + to_z[dz] for dx, dy, dz in hops]
    for (dx, dy, dz), target in zip(hops, targets):
        if (dx > 0) + (dy > 0) + (dz > 0) == 1:
            pl.semaphore_signal(barrier, inc=1, device_id=at_chip(target), device_id_type=MESH)

    window = pl.multiple_of(lax.div(seg, 2) * 8, 8)
    loads = [
        pltpu.make_async_copy(src, dst, load_sem.at[n])
        for n, (src, dst) in enumerate(
            (
                (key_h, key_v),
                (value_h, value_v),
                (weight_h, w_all.at[0, 0, 0]),
                (filt_h.at[pl.ds(window, WIN), :], filt_v),
                (narrow_h, narrow),
                (twiddle_h, twiddle),
                (wide_h, wide),
                (gate_h, gate_v),
                (skip_h, skip_s),
            )
        )
    ]
    for load in loads:
        load.start()

    def rcopy(src, dst, send, recv, device):
        return pltpu.make_async_remote_copy(
            src_ref=src, dst_ref=dst, send_sem=send, recv_sem=recv, device_id=device, device_id_type=MESH
        )

    loads[0].wait()
    loads[1].wait()

    def mix(j, carry):
        cols = pl.ds(pl.multiple_of(j * L, L), L)
        product = key_v[:, cols].astype(f32) * value_v[:, cols].astype(f32)
        strip[pl.ds(j, HERE, stride=PITCH), :] = product
        return carry

    lax.fori_loop(0, TILES, mix, 0, unroll=4)
    for c in range(HERE):
        mixed_b[c] = strip[c * PITCH : c * PITCH + TILES, :].astype(bf16)

    pl.semaphore_wait(barrier, SEGS - 1 + 2 + NX - 1 + NY - 1 + NZ - 1)

    seg_rows = pl.ds(pl.multiple_of(seg * TILES, TILES), TILES)

    def x_copy(p, step):
        return rcopy(
            mixed_b.at[pl.ds(at_seg(step) * OWN + 2 * p, 2)],
            x_in.at[pl.ds(2 * p, 2), seg_rows, :],
            x_send.at[3 * p + step - 1],
            x_recv.at[3 * p + step - 1],
            (at_seg(step), ch),
        )

    left, right = pl.ds(0, HALF), pl.ds(HALF, HALF)
    sides = (at_chip(beside), across)

    def z_pair(there, here, n):
        return [
            rcopy(here[m], there[m], w1_send.at[2 * n + m], w1_recv.at[2 * n + m], sides[m]) for m in range(2)
        ]

    def z_stage(n, *slots):
        return z_pair([w_all.at[(1, *slot)] for slot in slots], [w_all.at[(0, *slot)] for slot in slots], n)

    every = slice(None)
    z_copies = z_stage(0, (0, 0, every, left), (0, 0, every, right))
    z_far = z_stage(1, (0, 2), (2, 0))
    z_rest = z_stage(2, (2, slice(1, NX), every, left), (slice(1, NY), 2, every, right))

    def x_peer(step):
        return at_chip((lax.rem(cx + step, NX) * NY + cy) * NZ + cz)

    def y_peer(step):
        return at_chip((cx * NY + lax.rem(cy + step, NY)) * NZ + cz)

    def first_copies(z, steps, send, recv):
        own = w_all.at[z, 0, 0]
        return [
            rcopy(own, w_all.at[z, 0, NX - step], send.at[step - 1], recv.at[step - 1], x_peer(step))
            for step in steps
        ] + [
            rcopy(own, w_all.at[z, NY - step, 0], send.at[step + 2], recv.at[step + 2], y_peer(step))
            for step in steps
        ]

    def second_copies(z, steps, send, recv):
        along_x, along_y = w_all.at[z, 0, 1:, :, left], w_all.at[z, 1:, 0, :, right]
        return [
            rcopy(along_x, w_all.at[z, NY - step, 1:, :, left], send.at[step - 1], recv.at[step - 1], y_peer(step))
            for step in steps
        ] + [
            rcopy(along_y, w_all.at[z, 1:, NX - step, :, right], send.at[step + 2], recv.at[step + 2], x_peer(step))
            for step in steps
        ]

    loads[2].wait()
    w_a = first_copies(0, ALL, w2_send, w2_recv)
    for copy in z_copies:
        copy.start()
    def x_start(*pairs):
        for p in pairs:
            for step in FAR_FIRST:
                x_copy(p, step).start()

    @pl.when(core == 0)
    def _():
        x_start(0)
        x_start(1, 2)

    for copy in w_a:
        copy.start()
    x_in[:, seg_rows, :] = mixed_b[pl.ds(seg * OWN, OWN)]

    loads[3].wait()
    for n in (4, 5, 6):
        loads[n].wait()

    def turn(j, carry):
        filt_x[pl.ds(j, WIN, stride=KPITCH), :] = filt_v[:, pl.ds(pl.multiple_of(j * L, L), L)]
        return carry

    lax.fori_loop(0, T // L, turn, 0, unroll=4)

    @pl.when(core == 1)
    def _():
        x_start(0)

    first = seg * OWN - window
    b_re, b_im = twiddle.at[:L, :], twiddle.at[L:, :]

    def spread(u, n):
        u_re, u_im = u[:L, n * L : (n + 1) * L], u[L:, n * L : (n + 1) * L]
        re, im = b_re[...], b_im[...]
        return jnp.concatenate([u_re * re - u_im * im, u_re * im + u_im * re], axis=1)

    def filter_spectrum(p, carry):
        strips = [
            filt_x[pl.ds(pl.multiple_of((first + 2 * p + n) * KPITCH, 8), T // L), :] for n in range(2)
        ]
        high, low = split(jnp.concatenate(strips, axis=1))
        a_high = narrow[: 2 * L, :]
        u = dot(a_high, high) + dot(narrow[2 * L :, :], high) + dot(a_high, low)
        v_high, v_low = split(jnp.concatenate([spread(u, n) for n in range(2)], axis=0))
        d_high = wide[: 2 * L, :]
        spectrum[p] = dot(v_high, d_high) + dot(v_low, d_high) + dot(v_high, wide[2 * L : 4 * L, :])
        return carry

    lax.fori_loop(0, PAIRS, filter_spectrum, 0)

    @pl.when(core == 1)
    def _():
        x_start(1, 2)

    for copy in z_copies:
        copy.wait_recv()
    w_c = first_copies(1, NEAR, w4_send, w4_recv)
    for copy in w_c:
        copy.start()
    for copy in w_a:
        copy.wait_recv()
    w_b = second_copies(0, ALL, w3_send, w3_recv)
    for copy in w_b + z_far:
        copy.start()

    def b_copy(p, step):
        rows = pl.ds(pl.multiple_of(at_seg(step) * TILES, TILES), TILES)
        return rcopy(
            conv_out.at[pl.ds(2 * p, 2), rows, :],
            conv_in.at[pl.ds(seg * OWN + 2 * p, 2)],
            b_send.at[3 * p + step - 1],
            b_recv.at[3 * p + step - 1],
            (at_seg(step), ch),
        )

    def convolve(p):
        pair = range(2)
        us = [dot(narrow[: 2 * L, :], x_in[2 * p + n]) for n in pair]
        xs = [dot(spread(u, 0).astype(bf16), wide[: 2 * L, :]) for u in us]
        zs = []
        for n in pair:
            h, x = spectrum[p, n * L : (n + 1) * L, :], xs[n]
            x_re, x_im, h_re, h_im = x[:, :L], x[:, L:], h[:, :L], h[:, L:]
            zs.append(jnp.concatenate([x_re * h_re - x_im * h_im, x_re * h_im + x_im * h_re], axis=1))
        es = [dot(z.astype(bf16), wide[4 * L : 6 * L, :]) for z in zs]
        fs = []
        for e in es:
            e_re, e_im, re, im = e[:, :L], e[:, L:], b_re[...], b_im[...]
            fs.append(jnp.concatenate([e_re * re + e_im * im, e_im * re - e_re * im], axis=0).astype(bf16))
        for n in pair:
            conv_out[2 * p + n] = dot(wide[6 * L :, :], fs[n]).astype(bf16)

    for p in range(PAIRS):
        for step in range(1, SEGS):
            x_copy(p, step).wait_recv()
        convolve(p)
        for step in FAR_FIRST:
            b_copy(p, step).start()
    for copy in w_c + z_far:
        copy.wait_recv()
    w_d = second_copies(1, NEAR, w5_send, w5_recv)
    for copy in w_d:
        copy.start()
    conv_in[pl.ds(seg * OWN, OWN)] = conv_out[:, seg_rows, :]

    loads[7].wait()
    loads[8].wait()
    for c in range(HERE):
        skip_v[c : c + 1, :] = jnp.full((1, L), skip_s[c], f32)

    for p in range(PAIRS):
        for step in range(1, SEGS):
            b_copy(p, step).wait_recv()
        for c in range(HERE):
            if c % OWN // 2 == p:
                strip[c * PITCH : c * PITCH + TILES, :] = conv_in[c].astype(f32)

    def gate_tile(j):
        cols = pl.ds(pl.multiple_of(j * L, L), L)
        mixed = key_v[:, cols].astype(f32) * value_v[:, cols].astype(f32)
        conv = strip[pl.ds(j, HERE, stride=PITCH), :]
        return (gate_v[:, cols].astype(f32) * (conv + skip_v[...] * mixed)).astype(bf16)

    gathered[:HERE, :] = gate_tile(chip)
    sends = []
    for n, (dx, dy, dz) in enumerate(hops):
        target = targets[n]
        slot = (dz * NY + (NY - dy) % NY) * NX + (NX - dx) % NX
        outgoing[n] = gate_tile(target)
        sends.append(
            rcopy(
                outgoing.at[n], gathered.at[slot * HERE : (slot + 1) * HERE, :], g_send, g_recv, at_chip(target)
            )
        )
        if n:
            sends[n - 1].start()
    sends[-1].start()

    for copy in w_b:
        copy.wait_recv()
    for copy in z_rest:
        copy.start()

    def wait_bytes(ref, sem):
        pltpu.make_async_copy(ref, ref, sem).wait()

    for copy in w_d + z_rest:
        copy.wait_recv()
    others = pl.ds(HERE, (CHIPS - 1) * HERE)
    wait_bytes(gathered.at[others, :], g_recv)

    def p_copy(n):
        cols = pl.ds(n * COLS, COLS)
        return rcopy(
            leaving.at[1 - core, :, cols],
            partner.at[:, cols],
            p_send.at[n],
            p_recv.at[n],
            other_core,
        )

    rows_here = L // CORES
    turned = gathered[...].T
    for n in range(CHUNKS):
        cols = pl.ds(n * COLS, COLS)
        sums = lax.dot_general(
            turned,
            w_all[:, :, :, :, cols].reshape(CHIPS * HERE, COLS),
            (((1,), (0,)), ((), ())),
            preferred_element_type=f32,
        )
        partial[0, :, cols] = sums[:rows_here]
        partial[1, :, cols] = sums[rows_here:]
        leaving[0, :, cols] = sums[:rows_here].astype(bf16)
        leaving[1, :, cols] = sums[rows_here:].astype(bf16)
        if n:
            p_copy(n - 1).start()
    p_copy(CHUNKS - 1).start()
    for n in range(CHUNKS):
        cols = pl.ds(n * COLS, COLS)
        p_copy(n).wait_recv()
        out_ref[:, cols] = (partial[core, :, cols] + partner[:, cols].astype(f32)).astype(bf16)

    for p in range(PAIRS):
        for step in range(1, SEGS):
            x_copy(p, step).wait_send()
            b_copy(p, step).wait_send()
    for copy in z_copies + z_far + z_rest + w_a + w_b + w_c + w_d:
        copy.wait_send()
    wait_bytes(gathered.at[others, :], g_send)
    for n in range(CHUNKS):
        p_copy(n).wait_send()


def on_device(*args):
    anywhere = pl.BlockSpec(memory_space=pltpu.HBM)
    wide, narrow, twiddle = tables()
    dma = pltpu.SemaphoreType.DMA
    return pl.pallas_call(
        kernel,
        out_shape=pltpu.VMEM((L // CORES, D), bf16),
        in_specs=[anywhere] * 9,
        out_specs=pl.BlockSpec(memory_space=pltpu.VMEM),
        scratch_shapes=[
            pltpu.VMEM((HERE, LOCAL), bf16),
            pltpu.VMEM((HERE, LOCAL), bf16),
            pltpu.VMEM((HERE, LOCAL), bf16),
            pltpu.VMEM((WIN, T), f32),
            pltpu.VMEM(wide.shape, bf16),
            pltpu.VMEM(narrow.shape, bf16),
            pltpu.VMEM(twiddle.shape, f32),
            pltpu.SMEM((HERE,), f32),
            pltpu.VMEM((HERE * PITCH, L), f32),
            pltpu.VMEM((HERE, TILES, L), bf16),
            pltpu.VMEM((OWN, T // L, L), bf16),
            pltpu.VMEM((WIN * KPITCH, L), f32),
            pltpu.VMEM((PAIRS, 2 * L, 2 * L), f32),
            pltpu.VMEM((OWN, T // L, L), bf16),
            pltpu.VMEM((HERE, TILES, L), bf16),
            pltpu.VMEM((HERE, L), f32),
            pltpu.VMEM((CHIPS, HERE, L), bf16),
            pltpu.VMEM((CHIPS * HERE, L), bf16),
            pltpu.VMEM((NZ, NY, NX, HERE, D), bf16),
            pltpu.VMEM((CORES, L // CORES, D), f32),
            pltpu.VMEM((CORES, L // CORES, D), bf16),
            pltpu.VMEM((L // CORES, D), bf16),
            dma((9,)), dma((9,)), dma((9,)), dma((9,)), dma((9,)), dma((6,)), dma((6,)),
            dma((6,)), dma((6,)), dma((6,)), dma((6,)), dma((6,)), dma((6,)), dma((6,)), dma((6,)),
            dma, dma, dma((CHUNKS,)), dma((CHUNKS,)),
        ],
        compiler_params=pltpu.CompilerParams(
            collective_id=0, has_side_effects=True, vmem_limit_bytes=60 * 1024 * 1024
        ),
        name="layer",
    )(*args, jnp.asarray(wide), jnp.asarray(narrow), jnp.asarray(twiddle))


def solution(mesh):
    return jax.shard_map(
        on_device,
        mesh=mesh,
        in_specs=(P("ch", "seg"), P("ch", "seg"), P("ch", "seg"), P("ch", None), P("ch"), P("ch", None)),
        out_specs=P(("seg", "ch"), None),
        check_vma=False,
    )
```

```python
import math

import jax
import jax.numpy as jnp
import numpy as np
from jax import lax
from jax.experimental import pallas as pl
from jax.experimental.pallas import tpu as pltpu
from jax.sharding import PartitionSpec as P

MESH = pl.DeviceIdType.MESH
f32, bf16 = jnp.float32, jnp.bfloat16

SEGS = 4
NX, NY, NZ, CORES = 4, 4, 2, 2
CHIPS = NX * NY * NZ
L = 128
D = 1536
HERE = 24
OWN = HERE // SEGS
LOCAL = 4096
T = SEGS * LOCAL
TILES = LOCAL // L
PITCH = TILES + 8
KPITCH = T // L + 8
WIN = 16
CHUNKS = 2
COLS = D // CHUNKS
HALF = D // 2
PAIRS = OWN // 2
FAR_FIRST = (2, 1, 3)
ALL, NEAR = (1, 2, 3), (1, 3)


def halves(table):
    high = table.astype(jnp.bfloat16)
    low = (table - high.astype(np.float32)).astype(jnp.bfloat16)
    return high, low


def tables():
    i = np.arange(L)
    outer = np.exp(-2j * np.pi * np.outer(i + 0.25, i) / L)
    twist = np.exp(-2j * np.pi * np.outer(i + 0.25, i) / T)
    inner = np.exp(-2j * np.pi * np.outer(i, i) / L)
    a2 = np.concatenate([outer.real, outer.imag], 0).astype(np.float32)
    d2 = np.block([[inner.real, inner.imag], [-inner.imag, inner.real]]).astype(np.float32)
    di = np.block([[inner.real, -inner.imag], [inner.imag, inner.real]]).astype(np.float32)
    a_high, a_low = halves(a2)
    d_high, d_low = halves(d2)
    back = (a2.T / T).astype(jnp.bfloat16)
    wide = np.concatenate([d_high, d_low, di.astype(jnp.bfloat16), back], 0)
    narrow = np.concatenate([a_high, a_low], 0)
    twiddle = np.concatenate([twist.real, twist.imag], 0).astype(np.float32)
    return wide, narrow, twiddle


def dot(a, b):
    return jnp.dot(a, b, preferred_element_type=f32)


def split(x):
    high = x.astype(bf16)
    return high, (x - high.astype(f32)).astype(bf16)


def kernel(
    gate_h, key_h, value_h, filt_h, skip_h, weight_h, wide_h, narrow_h, twiddle_h,
    out_ref,
    gate_v, key_v, value_v, filt_v, wide, narrow, twiddle,
    skip_s, strip, mixed_b, x_in, filt_x, spectrum, conv_out, conv_in, skip_v,
    outgoing, gathered, w_all, partial, leaving, partner,
    load_sem, x_send, x_recv, b_send, b_recv, w1_send, w1_recv,
    w2_send, w2_recv, w3_send, w3_recv, w4_send, w4_recv, w5_send, w5_recv,
    g_send, g_recv, p_send, p_recv,
):
    seg = lax.axis_index("seg")
    ch = lax.axis_index("ch")
    core = lax.rem(ch, CORES)
    chip = lax.div(ch, CORES)
    cx, cy, cz = lax.div(chip, NY * NZ), lax.rem(lax.div(chip, NZ), NY), lax.rem(chip, NZ)

    def at_seg(step):
        return lax.rem(seg + step, SEGS)

    def at_chip(other):
        return (seg, other * CORES + core)

    barrier = pltpu.get_barrier_semaphore()
    for step in range(1, SEGS):
        pl.semaphore_signal(barrier, inc=1, device_id=(at_seg(step), ch), device_id_type=MESH)
    other_core = (seg, chip * CORES + 1 - core)
    beside = chip + 1 - 2 * cz
    across = (lax.rem(seg + SEGS - 1 + 2 * cz, SEGS), beside * CORES + core)
    for device in (other_core, across):
        pl.semaphore_signal(barrier, inc=1, device_id=device, device_id_type=MESH)

    to_x = [lax.rem(cx + d, NX) * (NY * NZ) for d in range(NX)]
    to_y = [lax.rem(cy + d, NY) * NZ for d in range(NY)]
    to_z = [cz, 1 - cz]
    hops = sorted(
        ((dx, dy, dz) for dx in range(NX) for dy in range(NY) for dz in range(NZ) if dx or dy or dz),
        key=lambda d: -(min(d[0], NX - d[0]) + min(d[1], NY - d[1]) + d[2]),
    )
    targets = [to_x[dx] + to_y[dy] + to_z[dz] for dx, dy, dz in hops]
    for (dx, dy, dz), target in zip(hops, targets):
        if (dx > 0) + (dy > 0) + (dz > 0) == 1:
            pl.semaphore_signal(barrier, inc=1, device_id=at_chip(target), device_id_type=MESH)

    window = pl.multiple_of(lax.div(seg, 2) * 8, 8)
    loads = [
        pltpu.make_async_copy(src, dst, load_sem.at[n])
        for n, (src, dst) in enumerate(
            (
                (key_h, key_v),
                (value_h, value_v),
                (weight_h, w_all.at[0, 0, 0]),
                (filt_h.at[pl.ds(window, WIN), :], filt_v),
                (narrow_h, narrow),
                (twiddle_h, twiddle),
                (wide_h, wide),
                (gate_h, gate_v),
                (skip_h, skip_s),
            )
        )
    ]
    for load in loads:
        load.start()

    def rcopy(src, dst, send, recv, device):
        return pltpu.make_async_remote_copy(
            src_ref=src, dst_ref=dst, send_sem=send, recv_sem=recv, device_id=device, device_id_type=MESH
        )

    loads[0].wait()
    loads[1].wait()

    def mix(j, carry):
        cols = pl.ds(pl.multiple_of(j * L, L), L)
        product = key_v[:, cols].astype(f32) * value_v[:, cols].astype(f32)
        strip[pl.ds(j, HERE, stride=PITCH), :] = product
        return carry

    lax.fori_loop(0, TILES, mix, 0, unroll=4)
    for c in range(HERE):
        mixed_b[c] = strip[c * PITCH : c * PITCH + TILES, :].astype(bf16)

    pl.semaphore_wait(barrier, SEGS - 1 + 2 + NX - 1 + NY - 1 + NZ - 1)

    seg_rows = pl.ds(pl.multiple_of(seg * TILES, TILES), TILES)

    def x_copy(p, step):
        return rcopy(
            mixed_b.at[pl.ds(at_seg(step) * OWN + 2 * p, 2)],
            x_in.at[pl.ds(2 * p, 2), seg_rows, :],
            x_send.at[3 * p + step - 1],
            x_recv.at[3 * p + step - 1],
            (at_seg(step), ch),
        )

    left, right = pl.ds(0, HALF), pl.ds(HALF, HALF)
    sides = (at_chip(beside), across)

    def z_pair(there, here, n):
        return [
            rcopy(here[m], there[m], w1_send.at[2 * n + m], w1_recv.at[2 * n + m], sides[m]) for m in range(2)
        ]

    def z_stage(n, *slots):
        return z_pair([w_all.at[(1, *slot)] for slot in slots], [w_all.at[(0, *slot)] for slot in slots], n)

    every = slice(None)
    z_copies = z_stage(0, (0, 0, every, left), (0, 0, every, right))
    z_far = z_stage(1, (0, 2), (2, 0))
    z_rest = z_stage(2, (2, slice(1, NX), every, left), (slice(1, NY), 2, every, right))

    def x_peer(step):
        return at_chip((lax.rem(cx + step, NX) * NY + cy) * NZ + cz)

    def y_peer(step):
        return at_chip((cx * NY + lax.rem(cy + step, NY)) * NZ + cz)

    def first_copies(z, steps, send, recv):
        own = w_all.at[z, 0, 0]
        return [
            rcopy(own, w_all.at[z, 0, NX - step], send.at[step - 1], recv.at[step - 1], x_peer(step))
            for step in steps
        ] + [
            rcopy(own, w_all.at[z, NY - step, 0], send.at[step + 2], recv.at[step + 2], y_peer(step))
            for step in steps
        ]

    def second_copies(z, steps, send, recv):
        along_x, along_y = w_all.at[z, 0, 1:, :, left], w_all.at[z, 1:, 0, :, right]
        return [
            rcopy(along_x, w_all.at[z, NY - step, 1:, :, left], send.at[step - 1], recv.at[step - 1], y_peer(step))
            for step in steps
        ] + [
            rcopy(along_y, w_all.at[z, 1:, NX - step, :, right], send.at[step + 2], recv.at[step + 2], x_peer(step))
            for step in steps
        ]

    loads[2].wait()
    w_a = first_copies(0, ALL, w2_send, w2_recv)
    for copy in z_copies + w_a:
        copy.start()
    def x_start(*pairs):
        for p in pairs:
            for step in FAR_FIRST:
                x_copy(p, step).start()

    @pl.when(core == 0)
    def _():
        x_start(0)
        x_start(1, 2)

    x_in[:, seg_rows, :] = mixed_b[pl.ds(seg * OWN, OWN)]

    loads[3].wait()
    for n in (4, 5, 6):
        loads[n].wait()

    def turn(j, carry):
        filt_x[pl.ds(j, WIN, stride=KPITCH), :] = filt_v[:, pl.ds(pl.multiple_of(j * L, L), L)]
        return carry

    lax.fori_loop(0, T // L, turn, 0, unroll=4)

    @pl.when(core == 1)
    def _():
        x_start(0)

    first = seg * OWN - window
    b_re, b_im = twiddle.at[:L, :], twiddle.at[L:, :]

    def spread(u, n):
        u_re, u_im = u[:L, n * L : (n + 1) * L], u[L:, n * L : (n + 1) * L]
        re, im = b_re[...], b_im[...]
        return jnp.concatenate([u_re * re - u_im * im, u_re * im + u_im * re], axis=1)

    def filter_spectrum(p, carry):
        strips = [
            filt_x[pl.ds(pl.multiple_of((first + 2 * p + n) * KPITCH, 8), T // L), :] for n in range(2)
        ]
        high, low = split(jnp.concatenate(strips, axis=1))
        a_high = narrow[: 2 * L, :]
        u = dot(a_high, high) + dot(narrow[2 * L :, :], high) + dot(a_high, low)
        v_high, v_low = split(jnp.concatenate([spread(u, n) for n in range(2)], axis=0))
        d_high = wide[: 2 * L, :]
        spectrum[p] = dot(v_high, d_high) + dot(v_low, d_high) + dot(v_high, wide[2 * L : 4 * L, :])
        return carry

    lax.fori_loop(0, PAIRS, filter_spectrum, 0)

    @pl.when(core == 1)
    def _():
        x_start(1)

    for copy in z_copies:
        copy.wait_recv()
    w_c = first_copies(1, NEAR, w4_send, w4_recv)
    for copy in w_c:
        copy.start()
    @pl.when(core == 1)
    def _():
        x_start(2)

    for copy in w_a:
        copy.wait_recv()
    w_b = second_copies(0, ALL, w3_send, w3_recv)
    for copy in w_b + z_far:
        copy.start()

    def b_copy(p, step):
        rows = pl.ds(pl.multiple_of(at_seg(step) * TILES, TILES), TILES)
        return rcopy(
            conv_out.at[pl.ds(2 * p, 2), rows, :],
            conv_in.at[pl.ds(seg * OWN + 2 * p, 2)],
            b_send.at[3 * p + step - 1],
            b_recv.at[3 * p + step - 1],
            (at_seg(step), ch),
        )

    def convolve(p):
        pair = range(2)
        us = [dot(narrow[: 2 * L, :], x_in[2 * p + n]) for n in pair]
        xs = [dot(spread(u, 0).astype(bf16), wide[: 2 * L, :]) for u in us]
        zs = []
        for n in pair:
            h, x = spectrum[p, n * L : (n + 1) * L, :], xs[n]
            x_re, x_im, h_re, h_im = x[:, :L], x[:, L:], h[:, :L], h[:, L:]
            zs.append(jnp.concatenate([x_re * h_re - x_im * h_im, x_re * h_im + x_im * h_re], axis=1))
        es = [dot(z.astype(bf16), wide[4 * L : 6 * L, :]) for z in zs]
        fs = []
        for e in es:
            e_re, e_im, re, im = e[:, :L], e[:, L:], b_re[...], b_im[...]
            fs.append(jnp.concatenate([e_re * re + e_im * im, e_im * re - e_re * im], axis=0).astype(bf16))
        for n in pair:
            conv_out[2 * p + n] = dot(wide[6 * L :, :], fs[n]).astype(bf16)

    for p in range(PAIRS):
        for step in range(1, SEGS):
            x_copy(p, step).wait_recv()
        convolve(p)
        for step in FAR_FIRST:
            b_copy(p, step).start()
    for copy in w_c + z_far:
        copy.wait_recv()
    w_d = second_copies(1, NEAR, w5_send, w5_recv)
    for copy in w_d:
        copy.start()
    conv_in[pl.ds(seg * OWN, OWN)] = conv_out[:, seg_rows, :]

    loads[7].wait()
    loads[8].wait()
    for c in range(HERE):
        skip_v[c : c + 1, :] = jnp.full((1, L), skip_s[c], f32)

    for p in range(PAIRS):
        for step in range(1, SEGS):
            b_copy(p, step).wait_recv()
        for c in range(HERE):
            if c % OWN // 2 == p:
                strip[c * PITCH : c * PITCH + TILES, :] = conv_in[c].astype(f32)

    def gate_tile(j):
        cols = pl.ds(pl.multiple_of(j * L, L), L)
        mixed = key_v[:, cols].astype(f32) * value_v[:, cols].astype(f32)
        conv = strip[pl.ds(j, HERE, stride=PITCH), :]
        return (gate_v[:, cols].astype(f32) * (conv + skip_v[...] * mixed)).astype(bf16)

    gathered[:HERE, :] = gate_tile(chip)
    sends = []
    for n, (dx, dy, dz) in enumerate(hops):
        target = targets[n]
        slot = (dz * NY + (NY - dy) % NY) * NX + (NX - dx) % NX
        outgoing[n] = gate_tile(target)
        sends.append(
            rcopy(
                outgoing.at[n], gathered.at[slot * HERE : (slot + 1) * HERE, :], g_send, g_recv, at_chip(target)
            )
        )
        if n:
            sends[n - 1].start()
    sends[-1].start()

    for copy in w_b:
        copy.wait_recv()
    for copy in z_rest:
        copy.start()

    def wait_bytes(ref, sem):
        pltpu.make_async_copy(ref, ref, sem).wait()

    for copy in w_d + z_rest:
        copy.wait_recv()
    others = pl.ds(HERE, (CHIPS - 1) * HERE)
    wait_bytes(gathered.at[others, :], g_recv)

    def p_copy(n):
        cols = pl.ds(n * COLS, COLS)
        return rcopy(
            leaving.at[1 - core, :, cols],
            partner.at[:, cols],
            p_send.at[n],
            p_recv.at[n],
            other_core,
        )

    rows_here = L // CORES
    turned = gathered[...].T
    for n in range(CHUNKS):
        cols = pl.ds(n * COLS, COLS)
        sums = lax.dot_general(
            turned,
            w_all[:, :, :, :, cols].reshape(CHIPS * HERE, COLS),
            (((1,), (0,)), ((), ())),
            preferred_element_type=f32,
        )
        partial[0, :, cols] = sums[:rows_here]
        partial[1, :, cols] = sums[rows_here:]
        leaving[0, :, cols] = sums[:rows_here].astype(bf16)
        leaving[1, :, cols] = sums[rows_here:].astype(bf16)
        if n:
            p_copy(n - 1).start()
    p_copy(CHUNKS - 1).start()
    for n in range(CHUNKS):
        cols = pl.ds(n * COLS, COLS)
        p_copy(n).wait_recv()
        out_ref[:, cols] = (partial[core, :, cols] + partner[:, cols].astype(f32)).astype(bf16)

    for p in range(PAIRS):
        for step in range(1, SEGS):
            x_copy(p, step).wait_send()
            b_copy(p, step).wait_send()
    for copy in z_copies + z_far + z_rest + w_a + w_b + w_c + w_d:
        copy.wait_send()
    wait_bytes(gathered.at[others, :], g_send)
    for n in range(CHUNKS):
        p_copy(n).wait_send()


def on_device(*args):
    anywhere = pl.BlockSpec(memory_space=pltpu.HBM)
    wide, narrow, twiddle = tables()
    dma = pltpu.SemaphoreType.DMA
    return pl.pallas_call(
        kernel,
        out_shape=pltpu.VMEM((L // CORES, D), bf16),
        in_specs=[anywhere] * 9,
        out_specs=pl.BlockSpec(memory_space=pltpu.VMEM),
        scratch_shapes=[
            pltpu.VMEM((HERE, LOCAL), bf16),
            pltpu.VMEM((HERE, LOCAL), bf16),
            pltpu.VMEM((HERE, LOCAL), bf16),
            pltpu.VMEM((WIN, T), f32),
            pltpu.VMEM(wide.shape, bf16),
            pltpu.VMEM(narrow.shape, bf16),
            pltpu.VMEM(twiddle.shape, f32),
            pltpu.SMEM((HERE,), f32),
            pltpu.VMEM((HERE * PITCH, L), f32),
            pltpu.VMEM((HERE, TILES, L), bf16),
            pltpu.VMEM((OWN, T // L, L), bf16),
            pltpu.VMEM((WIN * KPITCH, L), f32),
            pltpu.VMEM((PAIRS, 2 * L, 2 * L), f32),
            pltpu.VMEM((OWN, T // L, L), bf16),
            pltpu.VMEM((HERE, TILES, L), bf16),
            pltpu.VMEM((HERE, L), f32),
            pltpu.VMEM((CHIPS, HERE, L), bf16),
            pltpu.VMEM((CHIPS * HERE, L), bf16),
            pltpu.VMEM((NZ, NY, NX, HERE, D), bf16),
            pltpu.VMEM((CORES, L // CORES, D), f32),
            pltpu.VMEM((CORES, L // CORES, D), bf16),
            pltpu.VMEM((L // CORES, D), bf16),
            dma((9,)), dma((9,)), dma((9,)), dma((9,)), dma((9,)), dma((6,)), dma((6,)),
            dma((6,)), dma((6,)), dma((6,)), dma((6,)), dma((6,)), dma((6,)), dma((6,)), dma((6,)),
            dma, dma, dma((CHUNKS,)), dma((CHUNKS,)),
        ],
        compiler_params=pltpu.CompilerParams(
            collective_id=0, has_side_effects=True, vmem_limit_bytes=60 * 1024 * 1024
        ),
        name="layer",
    )(*args, jnp.asarray(wide), jnp.asarray(narrow), jnp.asarray(twiddle))


def solution(mesh):
    return jax.shard_map(
        on_device,
        mesh=mesh,
        in_specs=(P("ch", "seg"), P("ch", "seg"), P("ch", "seg"), P("ch", None), P("ch"), P("ch", None)),
        out_specs=P(("seg", "ch"), None),
        check_vma=False,
    )
```
